8 devices in a mesh: data: 1 (over z), tp: 2 (over y), ep: 4 (over x, core).
Axes of the slice: x: 2, y: 2, z: 1, core: 2. Of those that a mesh axis runs over, the one named last changes fastest.
Arguments:
- tokens_a: bfloat16 [2048, 1280], P(('data', 'ep', 'tp'))
- tokens_b: bfloat16 [2048, 1280], P(('data', 'ep', 'tp'))
- experts_a: int32 [2048, 6], P(('data', 'ep', 'tp'))
- experts_b: int32 [2048, 6], P(('data', 'ep', 'tp'))
- gates_a: float32 [2048, 6], P(('data', 'ep', 'tp'))
- gates_b: float32 [2048, 6], P(('data', 'ep', 'tp'))
- slots_a: int32 [2048, 6], P(('data', 'ep', 'tp'))
- slots_b: int32 [2048, 6], P(('data', 'ep', 'tp'))
- shared_w1: bfloat16 [1280, 1792], P(None, 'tp')
- shared_w3: bfloat16 [1280, 1792], P(None, 'tp')
- shared_w2: bfloat16 [1792, 1280], P('tp')
- routed_w1: bfloat16 [64, 1280, 896], P('ep')
- routed_w3: bfloat16 [64, 1280, 896], P('ep')
- routed_w2: bfloat16 [64, 896, 1280], P('ep')
Outputs:
- output 1: bfloat16 [2048, 1280], P(('data', 'ep', 'tp'))
- output 2: bfloat16 [2048, 1280], P(('data', 'ep', 'tp'))
All inputs are finite; a program needn't handle non-finite values.
Results may differ from the reference program's by a relative error of at most 0.00608049.
Values are sent between devices in bfloat16 or wider.
A program may use at most 1 GiB of HBM per device.

```python
import jax
import jax.numpy as jnp
from jax import lax

TOK_DEV = 256
TP_SIZE = 2
EP_SIZE = 4
MODEL_DIM = 1280
EXPERTS = 64
TOP_K = 6
EXPERT_FF = 896
SHARED_FF = 1792
CAPACITY = 48

GROUP_DEVS = TP_SIZE * EP_SIZE
GROUP_TOK = GROUP_DEVS * TOK_DEV


def draw_routing(key):
    key_base, key_rank, key_tie = jax.random.split(key, 3)
    base = jax.random.randint(key_base, (GROUP_TOK, EXPERTS), 0, 64)
    rank_of = jax.random.permutation(key_rank, EXPERTS)
    favoured = jnp.where((rank_of >= 1) & (rank_of <= EXPERTS // 8), 6, 0)
    forced = jnp.where(rank_of == 0, 4096, 0)
    tok_ids = jnp.arange(GROUP_TOK)
    head_tok = (tok_ids % TOK_DEV) < CAPACITY
    cover = jnp.where(tok_ids[:, None] == jnp.arange(EXPERTS)[None, :], 4096, 0)
    score = base + favoured[None, :] + jnp.where(head_tok[:, None], forced[None, :], 0) + cover
    tie_rank = jax.random.permutation(key_tie, jnp.broadcast_to(jnp.arange(EXPERTS), (GROUP_TOK, EXPERTS)), axis=1, independent=True)
    chosen = lax.top_k(score * EXPERTS + tie_rank, TOP_K)[1]
    per_dev = chosen.reshape(GROUP_DEVS, TOK_DEV * TOP_K)
    one_hot = (per_dev[:, :, None] == jnp.arange(EXPERTS)[None, None, :]).astype(jnp.int32)
    earlier = jnp.cumsum(one_hot, axis=1) - one_hot
    position = jnp.sum(earlier * one_hot, axis=2)
    slots = jnp.where(position < CAPACITY, position, -1).reshape(GROUP_TOK, TOP_K)
    return chosen.astype(jnp.int32), slots.astype(jnp.int32)


def setup_inputs(seed: int = 0, part: int = 0) -> dict:
    key = jax.random.key(seed)
    part_keys = jax.random.split(jax.random.fold_in(key, part), 6)
    weight_keys = jax.random.split(key, 6)
    tokens_a = jax.random.normal(part_keys[0], (GROUP_TOK, MODEL_DIM), jnp.float32).astype(jnp.bfloat16)
    tokens_b = jax.random.normal(part_keys[1], (GROUP_TOK, MODEL_DIM), jnp.float32).astype(jnp.bfloat16)
    experts_a, slots_a = draw_routing(part_keys[2])
    experts_b, slots_b = draw_routing(part_keys[3])
    gates_a = jax.random.uniform(part_keys[4], (GROUP_TOK, TOP_K), jnp.float32, 0.5, 1.5) * TOP_K ** -0.5
    gates_b = jax.random.uniform(part_keys[5], (GROUP_TOK, TOP_K), jnp.float32, 0.5, 1.5) * TOP_K ** -0.5
    shared_w1 = (jax.random.normal(weight_keys[0], (MODEL_DIM, SHARED_FF), jnp.float32) * MODEL_DIM ** -0.5).astype(jnp.bfloat16)
    shared_w3 = (jax.random.normal(weight_keys[1], (MODEL_DIM, SHARED_FF), jnp.float32) * MODEL_DIM ** -0.5).astype(jnp.bfloat16)
    shared_w2 = (jax.random.normal(weight_keys[2], (SHARED_FF, MODEL_DIM), jnp.float32) * SHARED_FF ** -0.5).astype(jnp.bfloat16)
    routed_w1 = (jax.random.normal(weight_keys[3], (EXPERTS, MODEL_DIM, EXPERT_FF), jnp.float32) * MODEL_DIM ** -0.5).astype(jnp.bfloat16)
    routed_w3 = (jax.random.normal(weight_keys[4], (EXPERTS, MODEL_DIM, EXPERT_FF), jnp.float32) * MODEL_DIM ** -0.5).astype(jnp.bfloat16)
    routed_w2 = (jax.random.normal(weight_keys[5], (EXPERTS, EXPERT_FF, MODEL_DIM), jnp.float32) * EXPERT_FF ** -0.5).astype(jnp.bfloat16)
    return {'tokens_a': tokens_a, 'tokens_b': tokens_b, 'experts_a': experts_a, 'experts_b': experts_b, 'gates_a': gates_a, 'gates_b': gates_b, 'slots_a': slots_a, 'slots_b': slots_b, 'shared_w1': shared_w1, 'shared_w3': shared_w3, 'shared_w2': shared_w2, 'routed_w1': routed_w1, 'routed_w3': routed_w3, 'routed_w2': routed_w2}


def swiglu_rows(rows, w_in, w_gate, w_out):
    proj_in = jnp.dot(rows, w_in, preferred_element_type=jnp.float32)
    proj_gate = jnp.dot(rows, w_gate, preferred_element_type=jnp.float32)
    hidden = (jax.nn.silu(proj_in) * proj_gate).astype(jnp.bfloat16)
    return jnp.dot(hidden, w_out, preferred_element_type=jnp.float32)


def shared_expert(tokens, shared_w1, shared_w3, shared_w2):
    blocks = tokens.reshape(GROUP_DEVS, TOK_DEV, MODEL_DIM)
    result = lax.map(lambda token_block: swiglu_rows(token_block, shared_w1, shared_w3, shared_w2), blocks)
    return result.reshape(GROUP_TOK, MODEL_DIM)


def routed_experts(tokens, experts, gates, slots, routed_w1, routed_w3, routed_w2):
    tok_dev = tokens.reshape(GROUP_DEVS, TOK_DEV, MODEL_DIM).astype(jnp.float32)
    expert_dev = experts.reshape(GROUP_DEVS, TOK_DEV, TOP_K)
    slot_dev = slots.reshape(GROUP_DEVS, TOK_DEV, TOP_K)
    gate_dev = gates.reshape(GROUP_DEVS, TOK_DEV, TOP_K)
    slot_range = jnp.arange(CAPACITY)

    def one_expert(routed_acc, step_in):
        w_in, w_gate, w_out, expert = step_in
        hits = ((expert_dev == expert)[..., None] & (slot_dev[..., None] == slot_range)).astype(jnp.float32)
        place_mat = jnp.sum(hits, axis=2)
        gate_mat = jnp.sum(hits * gate_dev[..., None], axis=2)
        buffer_rows = jnp.einsum('ntc,ntd->ncd', place_mat, tok_dev).astype(jnp.bfloat16)
        expert_out = swiglu_rows(buffer_rows.reshape(GROUP_DEVS * CAPACITY, MODEL_DIM), w_in, w_gate, w_out).astype(jnp.bfloat16)
        expert_out = expert_out.reshape(GROUP_DEVS, CAPACITY, MODEL_DIM).astype(jnp.float32)
        return routed_acc + jnp.einsum('ntc,ncd->ntd', gate_mat, expert_out), None

    start_acc = jnp.zeros((GROUP_DEVS, TOK_DEV, MODEL_DIM), jnp.float32)
    routed_acc, unused = lax.scan(one_expert, start_acc, (routed_w1, routed_w3, routed_w2, jnp.arange(EXPERTS)))
    return routed_acc.reshape(GROUP_TOK, MODEL_DIM)


def one_microbatch(tokens, experts, gates, slots, shared_w1, shared_w3, shared_w2, routed_w1, routed_w3, routed_w2):
    shared_out = shared_expert(tokens, shared_w1, shared_w3, shared_w2)
    routed_out = routed_experts(tokens, experts, gates, slots, routed_w1, routed_w3, routed_w2)
    return (tokens.astype(jnp.float32) + shared_out + routed_out).astype(jnp.bfloat16)


def reference(tokens_a, tokens_b, experts_a, experts_b, gates_a, gates_b, slots_a, slots_b, shared_w1, shared_w3, shared_w2, routed_w1, routed_w3, routed_w2):
    out_a = one_microbatch(tokens_a, experts_a, gates_a, slots_a, shared_w1, shared_w3, shared_w2, routed_w1, routed_w3, routed_w2)
    out_b = one_microbatch(tokens_b, experts_b, gates_b, slots_b, shared_w1, shared_w3, shared_w2, routed_w1, routed_w3, routed_w2)
    return (out_a, out_b)
```

```python
import functools

import jax
import jax.numpy as jnp
from jax import lax
from jax.experimental import pallas as pl
from jax.experimental.pallas import tpu as pltpu
from jax.sharding import PartitionSpec as P

MESH = pl.DeviceIdType.MESH
BF16 = jnp.bfloat16
F32 = jnp.float32

TOK = 256
D = 1280
F = 896
TOP_K = 6
CAP = 48
EXP = 16
NSRC = 4
GRP = 4
COL = 256
NCOL = D // COL
ROWS = NSRC * CAP
SLOTS13 = 3


def dot(a, b):
    return jnp.dot(a, b, preferred_element_type=F32)


def kernel(xa, xb, meta, sw1, sw3, sw2, rw1, rw3, rw2,
           oa, ob, pw1, pw3, pw2,
           metabuf, tokbuf, slots, gmat, rowsg, hbuf, ybuf, hs, send1, send3, tmp0, tmp2, q0, q2, rr, w13, w2b,
           meta_s, meta_r, tc_s, tc_r, tx_s, tx_r, td_s, td_r, p1_s, p1_r, p3_s, p3_r, rr_s, rr_r,
           yw_s, yw_r, fw_s, fw_r, w13_s, w2_s, sw2_s):
    ep = lax.axis_index("ep")
    tp = lax.axis_index("tp")
    core = lax.rem(ep, 2)
    core_peer = {"ep": ep + 1 - 2 * core}
    x_peer = {"ep": lax.rem(ep + 2, 4)}
    diag = {"ep": 3 - ep}
    y_peer = {"tp": 1 - tp}
    own = (xa, xb)

    def remote(src, dst, s, r, dev):
        return pltpu.make_async_remote_copy(src_ref=src, dst_ref=dst, send_sem=s, recv_sem=r, device_id=dev, device_id_type=MESH)

    def w13_copies(u):
        slot = lax.rem(u, SLOTS13)
        e = lax.rem(u, EXP)
        return (pltpu.make_async_copy(rw1.at[e], w13.at[slot, 0], w13_s.at[slot, 0]),
                pltpu.make_async_copy(rw3.at[e], w13.at[slot, 1], w13_s.at[slot, 1]))

    def w2_copy(step, q):
        n = lax.rem(step, NCOL)
        return pltpu.make_async_copy(rw2.at[pl.ds(q * GRP, GRP), :, pl.ds(pl.multiple_of(n * COL, COL), COL)], w2b.at[q], w2_s.at[q])

    for u in range(SLOTS13):
        for cp in w13_copies(u):
            cp.start()

    barrier = pltpu.get_barrier_semaphore()
    for dev in (core_peer, x_peer, diag, y_peer):
        pl.semaphore_signal(barrier, inc=1, device_id=dev, device_id_type=MESH)
    pl.semaphore_wait(barrier, 4)

    meta_cp = [remote(meta, metabuf.at[i], meta_s.at[i], meta_r.at[i], dev) for i, dev in enumerate((core_peer, x_peer, diag))]
    x_cp = [remote(own[m], tokbuf.at[m, 1], tx_s.at[m], tx_r.at[m], x_peer) for m in range(2)]
    c_cp = [remote(own[m], tokbuf.at[m, 0], tc_s.at[m], tc_r.at[m], core_peer) for m in range(2)]
    d_cp = [remote(tokbuf.at[m, 1], tokbuf.at[m, 2], td_s.at[m], td_r.at[m], core_peer) for m in range(2)]
    for cp in meta_cp:
        cp.start()
    x_cp[0].start()
    c_cp[0].start()
    c_cp[1].start()

    half_d, half_f = D // 2, F // 2
    rows_d = pl.ds(pl.multiple_of(core * half_d, 128), half_d)
    rows_f = pl.ds(pl.multiple_of(core * half_f, 64), half_f)
    yw_cp = [remote(w.at[r], p.at[r], yw_s.at[i], yw_r.at[i], y_peer)
             for i, (w, p, r) in enumerate(((sw1, pw1, rows_d), (sw3, pw3, rows_d), (sw2, pw2, rows_f)))]
    fw_cp = [remote(p.at[r], p.at[r], fw_s.at[i], fw_r.at[i], core_peer)
             for i, (p, r) in enumerate(((pw1, rows_d), (pw3, rows_d), (pw2, rows_f)))]
    for cp in yw_cp:
        cp.start()
    for q in range(EXP // GRP):
        w2_copy(0, q).start()

    for cp in meta_cp:
        cp.wait()

    def route(i, carry):
        m, src = i // NSRC, lax.rem(i, NSRC)
        info = jnp.where(src == 0, meta[m], metabuf[lax.max(src, 1) - 1, m])
        first = ((ep * EXP + lax.broadcasted_iota(jnp.int32, (EXP, TOK), 0)) * CAP).astype(F32)
        slot = jnp.full((EXP, TOK), -1.0, F32)
        gate = jnp.zeros((EXP, TOK), F32)
        for j in range(TOP_K):
            s = info[j:j + 1, :] - first
            hit = (s >= 0.0) & (s < float(CAP))
            slot = jnp.where(hit, s, slot)
            gate = jnp.where(hit, info[TOP_K + j:TOP_K + j + 1, :], gate)
        pos = lax.broadcasted_iota(jnp.int32, (CAP, TOK), 0).astype(F32)
        for e in range(EXP):
            slots[m, src, e] = slot[e:e + 1, :]
        part = EXP // 2
        for k in range(2):
            g = jnp.concatenate([jnp.where(pos == slot[e:e + 1, :], gate[e:e + 1, :], 0.0)
                                 for e in range(k * part, (k + 1) * part)], axis=0).T
            hi = g.astype(BF16)
            g = g - hi.astype(F32)
            mid = g.astype(BF16)
            low = (g - mid.astype(F32)).astype(BF16)
            for p, v in enumerate((hi, mid, low)):
                gmat[m, src, :, pl.ds(p * EXP * CAP + k * part * CAP, part * CAP)] = v
        return carry

    lax.fori_loop(0, 2 * NSRC, route, 0)

    def arrive(m):
        c_cp[m].wait()
        x_cp[m].wait()
        d_cp[m].start()

    def swiglu_in(x, w1, w3, store):
        full = F // COL
        for k in range(full):
            cols = pl.ds(k * COL, COL)
            a = dot(x, w1[:, cols])
            b = dot(x, w3[:, cols])
            store(cols, (jax.nn.silu(a) * b).astype(BF16))
        cols = pl.ds(full * COL, F - full * COL)
        ab = dot(x, jnp.concatenate([w1[:, cols], w3[:, cols]], axis=1))
        a, b = ab[:, :F - full * COL], ab[:, F - full * COL:]
        store(cols, (jax.nn.silu(a) * b).astype(BF16))

    def phase1(m):
        toks = (own[m], tokbuf.at[m, 0], tokbuf.at[m, 1], tokbuf.at[m, 2])

        def group(g, carry):
            pos = lax.broadcasted_iota(jnp.int32, (CAP, TOK), 0).astype(F32)
            for src in range(NSRC):
                place = jnp.concatenate([jnp.where(pos == slots[m, src, g * GRP + i], 1.0, 0.0) for i in range(GRP)], axis=0).astype(BF16)
                for n in range(NCOL):
                    cols = pl.ds(n * COL, COL)
                    r = dot(place, toks[src][:, cols]).astype(BF16)
                    for i in range(GRP):
                        rowsg[i, pl.ds(src * CAP, CAP), cols] = r[i * CAP:(i + 1) * CAP]

            def expert(i, carry):
                u = m * EXP + g * GRP + i
                slot = lax.rem(u, SLOTS13)
                for cp in w13_copies(u):
                    cp.wait()
                e = g * GRP + i

                def store(cols, v):
                    hbuf[e, :, cols] = v

                swiglu_in(rowsg[i], w13.at[slot, 0], w13.at[slot, 1], store)

                @pl.when(u + SLOTS13 < 2 * EXP)
                def _():
                    for cp in w13_copies(u + SLOTS13):
                        cp.start()
                return carry

            return lax.fori_loop(0, GRP, expert, carry)

        lax.fori_loop(0, EXP // GRP, group, 0)

    def sum_copies(step, m=None):
        par = lax.rem(step, 2)
        return (remote(send1.at[par], q0.at[step], p1_s.at[step], p1_r.at[step], core_peer),
                remote(send3.at[par], q2.at[step], p3_s.at[step], p3_r.at[step], core_peer),
                remote(q2.at[step], rr.at[step], rr_s.at[step], rr_r.at[step], x_peer))

    def phase2(m):
        def column(n, carry):
            step = m * NCOL + n
            par = lax.rem(step, 2)
            for q in range(EXP // GRP):
                w2_copy(step, q).wait()
                for i in range(GRP):
                    e = q * GRP + i
                    y = dot(hbuf[e], w2b[q, i]).astype(BF16)
                    for src in range(NSRC):
                        ybuf[src, e] = y[src * CAP:(src + 1) * CAP]

                @pl.when(step + 1 < 2 * NCOL)
                def _():
                    w2_copy(step + 1, q).start()

            def combine(src):
                y = ybuf[src].reshape(EXP * CAP, COL)
                k = EXP * CAP
                g = gmat.at[m, src]
                return dot(g[:, :k], y) + dot(g[:, k:2 * k], y) + dot(g[:, 2 * k:], y)

            @pl.when(step >= 2)
            def _():
                old1, old3, _unused = sum_copies(step - 2)
                old1.wait_send()
                old3.wait_send()

            cp1, cp3, cpr = sum_copies(step)
            send3[par] = combine(3)
            cp3.start()
            tmp2[...] = combine(2)
            send1[par] = combine(1)
            cp1.start()
            tmp0[...] = combine(0)
            cp3.wait_recv()
            q2[step] = q2[step] + tmp2[...]
            cpr.start()
            cp1.wait_recv()
            q0[step] = q0[step] + tmp0[...]
            return carry

        lax.fori_loop(0, NCOL, column, 0)

    arrive(0)
    x_cp[1].start()
    d_cp[0].wait()
    phase1(0)
    arrive(1)
    phase2(0)
    d_cp[1].wait()
    phase1(1)

    local13 = (pltpu.make_async_copy(sw1, w13.at[2, 0], w13_s.at[2, 0]), pltpu.make_async_copy(sw3, w13.at[2, 1], w13_s.at[2, 1]))
    peer13 = (pltpu.make_async_copy(pw1, w13.at[0, 0], w13_s.at[0, 0]), pltpu.make_async_copy(pw3, w13.at[0, 1], w13_s.at[0, 1]))
    for cp in local13:
        cp.start()
    for i in range(2):
        yw_cp[i].wait()
        fw_cp[i].start()
    phase2(1)
    for i in range(2):
        fw_cp[i].wait()
        peer13[i].start()
    yw_cp[2].wait()
    fw_cp[2].start()

    def shared_in(half, slot):
        for m in range(2):
            def store(cols, v):
                hs[half, pl.ds(m * TOK, TOK), cols] = v

            swiglu_in(own[m][...], w13.at[slot, 0], w13.at[slot, 1], store)

    for cp in local13:
        cp.wait()
    shared_in(0, 2)
    fw_cp[2].wait()

    def sw2_copies(n):
        cols = pl.ds(n * COL, COL)
        slot = n % GRP
        return (pltpu.make_async_copy(sw2.at[:, cols], w2b.at[slot, 0], sw2_s.at[slot, 0]),
                pltpu.make_async_copy(pw2.at[:, cols], w2b.at[slot, 1], sw2_s.at[slot, 1]))

    for n in range(GRP):
        for cp in sw2_copies(n):
            cp.start()
    for cp in peer13:
        cp.wait()
    shared_in(1, 0)
    for n in range(NCOL):
        for cp in sw2_copies(n):
            cp.wait()
        cols = pl.ds(n * COL, COL)
        for m in range(2):
            rows = pl.ds(m * TOK, TOK)
            s = dot(hs[0, rows, :], w2b[n % GRP, 0]) + dot(hs[1, rows, :], w2b[n % GRP, 1])
            q0[m * NCOL + n] = q0[m * NCOL + n] + s + own[m][:, cols].astype(F32)
        if n + GRP < NCOL:
            for cp in sw2_copies(n + GRP):
                cp.start()
    for m, out in enumerate((oa, ob)):
        for n in range(NCOL):
            step = m * NCOL + n
            sum_copies(step)[2].wait()
            out[:, pl.ds(n * COL, COL)] = (q0[step] + rr[step]).astype(BF16)
    for step in range(2 * NCOL - 2, 2 * NCOL):
        cp1, cp3, _unused = sum_copies(step)
        cp1.wait_send()
        cp3.wait_send()


def solution(mesh):
    tok_spec = P(('data', 'ep', 'tp'), None)
    in_specs = (tok_spec,) * 8 + (P(None, 'tp'), P(None, 'tp'), P('tp', None), P('ep', None, None), P('ep', None, None), P('ep', None, None))

    def layer_local(tokens_a, tokens_b, experts_a, experts_b, gates_a, gates_b, slots_a, slots_b,
                    shared_w1, shared_w3, shared_w2, routed_w1, routed_w3, routed_w2):
        def info(experts, gates, slots):
            row = jnp.where(slots >= 0, experts * CAP + slots, -1).astype(F32)
            return jnp.concatenate([row.T, gates.T], axis=0)

        meta = jnp.stack([info(experts_a, gates_a, slots_a), info(experts_b, gates_b, slots_b)])
        vmem = pl.BlockSpec(memory_space=pltpu.VMEM)
        hbm = pl.BlockSpec(memory_space=pltpu.HBM)
        sem = pltpu.SemaphoreType.DMA
        steps = 2 * NCOL
        out = pl.pallas_call(
            kernel,
            name="moe_layer",
            out_shape=(jax.ShapeDtypeStruct((TOK, D), BF16), jax.ShapeDtypeStruct((TOK, D), BF16),
                       jax.ShapeDtypeStruct((D, F), BF16), jax.ShapeDtypeStruct((D, F), BF16), jax.ShapeDtypeStruct((F, D), BF16)),
            in_specs=[vmem] * 3 + [hbm] * 6,
            out_specs=(vmem, vmem, hbm, hbm, hbm),
            scratch_shapes=[
                pltpu.VMEM((3, 2, 2 * TOP_K, TOK), F32),
                pltpu.VMEM((2, 3, TOK, D), BF16),
                pltpu.VMEM((2, NSRC, EXP, 1, TOK), F32),
                pltpu.VMEM((2, NSRC, TOK, 3 * EXP * CAP), BF16),
                pltpu.VMEM((GRP, ROWS, D), BF16),
                pltpu.VMEM((EXP, ROWS, F), BF16),
                pltpu.VMEM((NSRC, EXP, CAP, COL), BF16),
                pltpu.VMEM((2, 2 * TOK, F), BF16),
                pltpu.VMEM((2, TOK, COL), F32),
                pltpu.VMEM((2, TOK, COL), F32),
                pltpu.VMEM((TOK, COL), F32),
                pltpu.VMEM((TOK, COL), F32),
                pltpu.VMEM((steps, TOK, COL), F32),
                pltpu.VMEM((steps, TOK, COL), F32),
                pltpu.VMEM((steps, TOK, COL), F32),
                pltpu.VMEM((SLOTS13, 2, D, F), BF16),
                pltpu.VMEM((EXP // GRP, GRP, F, COL), BF16),
                sem((3,)), sem((3,)), sem((2,)), sem((2,)), sem((2,)), sem((2,)), sem((2,)), sem((2,)),
                sem((steps,)), sem((steps,)), sem((steps,)), sem((steps,)), sem((steps,)), sem((steps,)),
                sem((3,)), sem((3,)), sem((3,)), sem((3,)), sem((SLOTS13, 2)), sem((EXP // GRP,)), sem((EXP // GRP, 2)),
            ],
            compiler_params=pltpu.CompilerParams(collective_id=0, has_side_effects=True, vmem_limit_bytes=67043328),
        )(tokens_a, tokens_b, meta, shared_w1, shared_w3, shared_w2, routed_w1, routed_w3, routed_w2)
        return out[0], out[1]

    return jax.shard_map(layer_local, mesh=mesh, in_specs=in_specs, out_specs=(tok_spec, tok_spec), check_vma=False)
```

```python
import functools

import jax
import jax.numpy as jnp
from jax import lax
from jax.experimental import pallas as pl
from jax.experimental.pallas import tpu as pltpu
from jax.sharding import PartitionSpec as P

MESH = pl.DeviceIdType.MESH
BF16 = jnp.bfloat16
F32 = jnp.float32

TOK = 256
D = 1280
F = 896
TOP_K = 6
CAP = 48
EXP = 16
NSRC = 4
XP, DG, OWN, CP = range(NSRC)
GRP = 4
COL = 256
NCOL = D // COL
ROWS = NSRC * CAP
SIDE = 2 * CAP
SLOTS13 = 4
SLOTS2 = 3
HALF = EXP // 2


def dot(a, b):
    return jnp.dot(a, b, preferred_element_type=F32)


def kernel(xa, xb, ea, eb, ga, gb, sa, sb, sw1, sw3, sw2, rw1, rw3, rw2,
           oa, ob, pw1, pw3, pw2,
           ids, gates, tokbuf, slots, gmat, rowsg, hs, hfar, hnear, ybuf, send, tmp, q0, q2, rr, w13, w2b,
           own_s, meta_s, meta_r, fmeta_s, fmeta_r, tc_s, tc_r, tx_s, tx_r, td_s, td_r, p1_s, p1_r, p3_s, p3_r, rr_s, rr_r,
           yw_s, yw_r, fw_s, fw_r, w13_s, w2_s, sw2_s, out_s):
    ep = lax.axis_index("ep")
    tp = lax.axis_index("tp")
    core = lax.rem(ep, 2)
    core_peer = {"ep": ep + 1 - 2 * core}
    x_peer = {"ep": lax.rem(ep + 2, 4)}
    diag = {"ep": 3 - ep}
    y_peer = {"tp": 1 - tp}
    own = (xa, xb)

    def remote(src, dst, s, r, dev):
        return pltpu.make_async_remote_copy(src_ref=src, dst_ref=dst, send_sem=s, recv_sem=r, device_id=dev, device_id_type=MESH)

    def expert_of(u):
        return lax.rem(jnp.where(u < EXP, u, u + EXP - SLOTS13), EXP)

    def w13_copies(u):
        slot = lax.rem(u, SLOTS13)
        e = expert_of(u)
        return (pltpu.make_async_copy(rw1.at[e], w13.at[slot, 0], w13_s.at[slot, 0]),
                pltpu.make_async_copy(rw3.at[e], w13.at[slot, 1], w13_s.at[slot, 1]))

    def w2_copy(unit):
        slot = lax.rem(unit, SLOTS2)
        n = lax.rem(lax.div(unit, 2), NCOL)
        first = lax.rem(unit, 2) * HALF
        return pltpu.make_async_copy(rw2.at[pl.ds(first, HALF), :, pl.ds(pl.multiple_of(n * COL, COL), COL)], w2b.at[slot], w2_s.at[slot])

    routing = ((ea, sa, ga), (eb, sb, gb))

    def routing_slots(m, src):
        return ids.at[src, m, 0], ids.at[src, m, 1], gates.at[src, m]

    own_cp = [pltpu.make_async_copy(a, b, own_s.at[m, k]) for m in range(2)
              for k, (a, b) in enumerate(zip((*routing[m], own[m]), (*routing_slots(m, OWN), tokbuf.at[m, OWN])))]
    for cp in own_cp:
        cp.start()

    barrier = pltpu.get_barrier_semaphore()
    for dev in (core_peer, x_peer, diag, y_peer):
        pl.semaphore_signal(barrier, inc=1, device_id=dev, device_id_type=MESH)
    pl.semaphore_wait(barrier, 4)

    def routing_cp(m, k, src, dst, ss, rs, dev):
        return remote(src[k], routing_slots(m, dst)[k], ss.at[m, k], rs.at[m, k], dev)

    cmeta_cp = [[routing_cp(m, k, routing[m], CP, meta_s.at[0], meta_r.at[0], core_peer) for k in range(3)] for m in range(2)]
    xmeta_cp = [[routing_cp(m, k, routing[m], XP, meta_s.at[1], meta_r.at[1], x_peer) for k in range(3)] for m in range(2)]
    dmeta_cp = [[routing_cp(m, k, routing_slots(m, XP), DG, fmeta_s, fmeta_r, core_peer) for k in range(3)] for m in range(2)]
    part = TOK // 2
    x_cp = [[remote(own[m].at[pl.ds(k * part, part)], tokbuf.at[m, XP, pl.ds(k * part, part)], tx_s.at[m, k], tx_r.at[m, k], x_peer) for k in range(2)] for m in range(2)]
    d_cp = [[remote(tokbuf.at[m, XP, pl.ds(k * part, part)], tokbuf.at[m, DG, pl.ds(k * part, part)], td_s.at[m, k], td_r.at[m, k], core_peer) for k in range(2)] for m in range(2)]
    c_cp = [remote(own[m], tokbuf.at[m, CP], tc_s.at[m], tc_r.at[m], core_peer) for m in range(2)]
    for cp in (*xmeta_cp[0], *xmeta_cp[1], *cmeta_cp[0], *cmeta_cp[1], *x_cp[0], *c_cp):
        cp.start()
    local13 = (pltpu.make_async_copy(sw1, w13.at[SLOTS13 - 1, 0], w13_s.at[SLOTS13 - 1, 0]),
               pltpu.make_async_copy(sw3, w13.at[SLOTS13 - 1, 1], w13_s.at[SLOTS13 - 1, 1]))
    for cp in local13:
        cp.start()
    for u in range(SLOTS13 - 1):
        for cp in w13_copies(jnp.int32(u)):
            cp.start()

    half_d, half_f = D // 2, F // 2
    rows_d = pl.ds(pl.multiple_of(core * half_d, 128), half_d)
    rows_f = pl.ds(pl.multiple_of(core * half_f, 64), half_f)
    yw_cp = [remote(w.at[r], p.at[r], yw_s.at[i], yw_r.at[i], y_peer)
             for i, (w, p, r) in enumerate(((sw1, pw1, rows_d), (sw3, pw3, rows_d), (sw2, pw2, rows_f)))]
    fw_cp = [remote(p.at[r], p.at[r], fw_s.at[i], fw_r.at[i], core_peer)
             for i, (p, r) in enumerate(((pw1, rows_d), (pw3, rows_d), (pw2, rows_f)))]
    for cp in yw_cp:
        cp.start()
    for unit in range(SLOTS2):
        w2_copy(unit).start()

    for cp in own_cp:
        cp.wait()

    def route(i, carry):
        m, src = carry, i
        first = ep * EXP + lax.broadcasted_iota(jnp.int32, (EXP, TOK), 0)
        id_rows, slot_rows, gate_rows = ids[src, m, 0], ids[src, m, 1], gates[src, m]
        slot = jnp.full((EXP, TOK), -1, jnp.int32)
        gate = jnp.zeros((EXP, TOK), F32)
        for j in range(TOP_K):
            hit = (id_rows[j:j + 1, :] == first) & (slot_rows[j:j + 1, :] >= 0)
            slot = jnp.where(hit, slot_rows[j:j + 1, :], slot)
            gate = jnp.where(hit, gate_rows[j:j + 1, :], gate)
        pos = lax.broadcasted_iota(jnp.int32, (CAP, TOK), 0)
        for e in range(EXP):
            slots[m, src, e] = slot[e:e + 1, :]
        part = EXP // 2
        for k in range(2):
            g = jnp.concatenate([jnp.where(pos == slot[e:e + 1, :], gate[e:e + 1, :], 0.0)
                                 for e in range(k * part, (k + 1) * part)], axis=0).T
            hi = g.astype(BF16)
            g = g - hi.astype(F32)
            mid = g.astype(BF16)
            low = (g - mid.astype(F32)).astype(BF16)
            for p, v in enumerate((hi, mid, low)):
                gmat[m, src, :, pl.ds(p * EXP * CAP + k * part * CAP, part * CAP)] = v
        return carry

    def route_all(m):
        for cp in (*xmeta_cp[m], *cmeta_cp[m]):
            cp.wait()
        for cp in dmeta_cp[m]:
            cp.start()
        for cp in dmeta_cp[m]:
            cp.wait()
        lax.fori_loop(0, NSRC, route, jnp.int32(m))

    def arrive(m):
        c_cp[m].wait()
        for k in range(2):
            x_cp[m][k].wait()
            d_cp[m][k].start()

    def swiglu_in(x, w1, w3, store):
        full = F // COL
        for k in range(full):
            cols = pl.ds(k * COL, COL)
            a = dot(x, w1[:, cols])
            b = dot(x, w3[:, cols])
            store(cols, (jax.nn.silu(a) * b).astype(BF16))
        cols = pl.ds(full * COL, F - full * COL)
        ab = dot(x, jnp.concatenate([w1[:, cols], w3[:, cols]], axis=1))
        a, b = ab[:, :F - full * COL], ab[:, F - full * COL:]
        store(cols, (jax.nn.silu(a) * b).astype(BF16))

    def phase1(m, after_gather):
        def group(t, carry):
            g = lax.rem(t + m * (EXP // GRP - 1), EXP // GRP)
            pos = lax.broadcasted_iota(jnp.int32, (CAP, TOK), 0)
            for src in range(NSRC):
                place = jnp.concatenate([jnp.where(pos == slots[m, src, g * GRP + i], 1.0, 0.0) for i in range(GRP)], axis=0).astype(BF16)
                for n in range(NCOL):
                    cols = pl.ds(n * COL, COL)
                    r = dot(place, tokbuf[m, src, :, cols]).astype(BF16)
                    for i in range(GRP):
                        rowsg[i, pl.ds(src * CAP, CAP), cols] = r[i * CAP:(i + 1) * CAP]

            after_gather(t)

            def expert(i, carry):
                u = m * EXP + t * GRP + i
                slot = lax.rem(u, SLOTS13)
                rows = pl.ds(pl.multiple_of((g * GRP + i) * SIDE, SIDE), SIDE)
                near = pl.ds(pl.multiple_of((g * GRP + i) * ROWS + m * SIDE, SIDE), SIDE)

                @pl.when((u < EXP) | (u >= EXP + SLOTS13))
                def _():
                    for cp in w13_copies(u):
                        cp.wait()

                def store(cols, v):
                    hfar[rows, cols] = v[:SIDE]
                    hnear[near, cols] = v[SIDE:]

                swiglu_in(rowsg[i], w13.at[slot, 0], w13.at[slot, 1], store)
                nxt = u + SLOTS13

                @pl.when((nxt < EXP) | ((nxt >= EXP + SLOTS13) & (nxt < 2 * EXP)))
                def _():
                    for cp in w13_copies(nxt):
                        cp.start()
                return carry

            return lax.fori_loop(0, GRP, expert, carry)

        lax.fori_loop(0, EXP // GRP, group, 0)

    def expand(unit, first, h, sources):
        slot = lax.rem(unit, SLOTS2)
        size = sources * CAP
        for i in range(HALF):
            e = first + i
            y = dot(h[e * size:(e + 1) * size, :], w2b[slot, i]).astype(BF16)
            for k in range(sources):
                ybuf[k, e] = y[k * CAP:(k + 1) * CAP]

    def refill(unit):
        @pl.when(unit < 6 * NCOL)
        def _():
            w2_copy(unit).start()

    def combine(k, m, src):
        y = ybuf[k].reshape(EXP * CAP, COL)
        n = EXP * CAP
        g = gmat.at[m, src]
        return dot(g[:, :n], y) + dot(g[:, n:2 * n], y) + dot(g[:, 2 * n:], y)

    def far_copies(step):
        par = lax.rem(step, 2)
        return (remote(send.at[par], q2.at[step], p3_s.at[step], p3_r.at[step], core_peer),
                remote(q2.at[step], rr.at[step], rr_s.at[step], rr_r.at[step], x_peer))

    def near_copy(m, n):
        return remote(send.at[m], q0.at[m * NCOL + n], p1_s.at[m * NCOL + n], p1_r.at[m * NCOL + n], core_peer)

    def finish(step):
        cp, back = far_copies(step)
        cp.wait()
        q2[step] = q2[step] + tmp[lax.rem(step, 2)]
        back.start()

    def far(m):
        def column(n, carry):
            step = m * NCOL + n
            w2_copy(2 * step).wait()
            expand(2 * step, 0, hfar, 2)
            refill(2 * step + SLOTS2)
            w2_copy(2 * step + 1).wait()
            expand(2 * step + 1, HALF, hfar, 2)
            par = lax.rem(step, 2)
            send[par] = combine(DG, m, DG)
            tmp[par] = combine(XP, m, XP)
            far_copies(step)[0].start()
            refill(2 * step + 1 + SLOTS2)

            @pl.when(n >= 1)
            def _():
                finish(step - 1)
            return carry

        lax.fori_loop(0, NCOL, column, 0)

    def shared_in(half, slot):
        for m in range(2):
            def store(cols, v):
                hs_of(half, m)[:, cols] = v

            swiglu_in(tokbuf[m, OWN], w13.at[slot, 0], w13.at[slot, 1], store)

    def hs_of(half, m):
        rows = pl.ds(m * TOK, TOK)
        return hfar.at[rows, :] if half else hs.at[rows, :]

    route_all(0)
    route_all(1)
    for cp in local13:
        cp.wait()
    shared_in(0, SLOTS13 - 1)
    for cp in w13_copies(jnp.int32(SLOTS13 - 1)):
        cp.start()
    arrive(0)
    for cp in x_cp[1]:
        cp.start()
    for cp in d_cp[0]:
        cp.wait()
    phase1(0, lambda t: None)
    arrive(1)
    far(0)
    for cp in d_cp[1]:
        cp.wait()

    def between(t):
        @pl.when(t == 0)
        def _():
            finish(jnp.int32(NCOL - 1))

        @pl.when(t == 2)
        def _():
            for i in range(2):
                yw_cp[i].wait()
                fw_cp[i].start()

    phase1(1, between)

    peer13 = (pltpu.make_async_copy(pw1, w13.at[1, 0], w13_s.at[1, 0]), pltpu.make_async_copy(pw3, w13.at[1, 1], w13_s.at[1, 1]))

    def sw2_slot(half, n):
        return w13.at[2 + half, lax.div(n, 3), pl.ds(0, F), pl.ds(pl.multiple_of(lax.rem(n, 3) * COL, COL), COL)]

    def sw2_copy(half, n):
        return pltpu.make_async_copy((sw2, pw2)[half].at[:, pl.ds(pl.multiple_of(n * COL, COL), COL)], sw2_slot(half, n), sw2_s.at[n, half])

    for i in range(2):
        fw_cp[i].wait()
        peer13[i].start()
    far(1)
    for n in range(NCOL):
        sw2_copy(0, jnp.int32(n)).start()
    yw_cp[2].wait()
    fw_cp[2].start()
    finish(jnp.int32(2 * NCOL - 1))
    for cp in peer13:
        cp.wait()
    shared_in(1, 1)
    fw_cp[2].wait()
    for n in range(NCOL):
        sw2_copy(1, jnp.int32(n)).start()

    def near_finish(n):
        for m in range(2):
            near_copy(m, n).wait()
            q0[m * NCOL + n] = q0[m * NCOL + n] + tmp[m]

    def near_column(n, carry):
        step = 2 * NCOL + n
        w2_copy(2 * step).wait()
        expand(2 * step, 0, hnear, NSRC)
        refill(2 * step + SLOTS2)

        @pl.when(n >= 1)
        def _():
            near_finish(n - 1)

        w2_copy(2 * step + 1).wait()
        expand(2 * step + 1, HALF, hnear, NSRC)
        for m in range(2):
            send[m] = combine(2 * m + 1, m, CP)
        for m in range(2):
            tmp[m] = combine(2 * m, m, OWN)
        for m in range(2):
            near_copy(m, n).start()
        refill(2 * step + 1 + SLOTS2)
        for half in range(2):
            sw2_copy(half, n).wait()
        cols = pl.ds(pl.multiple_of(n * COL, COL), COL)
        for m in range(2):
            s = dot(hs_of(0, m)[...], sw2_slot(0, n)[...]) + dot(hs_of(1, m)[...], sw2_slot(1, n)[...])
            tmp[m] = tmp[m] + s + tokbuf[m, OWN, :, cols].astype(F32)
        return carry

    lax.fori_loop(0, NCOL, near_column, 0)
    near_finish(jnp.int32(NCOL - 1))

    out_cp = []
    for m, out in enumerate((oa, ob)):
        for n in range(NCOL):
            step = m * NCOL + n
            cols = pl.ds(n * COL, COL)
            far_copies(jnp.int32(step))[1].wait()
            tokbuf[m, XP, :, cols] = (q0[step] + rr[step]).astype(BF16)
            out_cp.append(pltpu.make_async_copy(tokbuf.at[m, XP, :, cols], out.at[:, cols], out_s.at[step]))
            out_cp[-1].start()
    for cp in out_cp:
        cp.wait()


def hand_over(a, b, oa, ob, buf, in_s, out_s):
    part = TOK // 4
    moves = [(src, dst, m, k) for m, (src, dst) in enumerate(((a, oa), (b, ob))) for k in range(4)]
    into = [pltpu.make_async_copy(src.at[pl.ds(k * part, part)], buf.at[m, pl.ds(k * part, part)], in_s.at[m, k]) for src, dst, m, k in moves]
    back = [pltpu.make_async_copy(buf.at[m, pl.ds(k * part, part)], dst.at[pl.ds(k * part, part)], out_s.at[m, k]) for src, dst, m, k in moves]
    for cp in into:
        cp.start()
    for i, o in zip(into, back):
        i.wait()
        o.start()
    for cp in back:
        cp.wait()


def solution(mesh):
    tok_spec = P(('data', 'ep', 'tp'), None)
    in_specs = (tok_spec,) * 8 + (P(None, 'tp'), P(None, 'tp'), P('tp', None), P('ep', None, None), P('ep', None, None), P('ep', None, None))

    def layer_local(tokens_a, tokens_b, experts_a, experts_b, gates_a, gates_b, slots_a, slots_b,
                    shared_w1, shared_w3, shared_w2, routed_w1, routed_w3, routed_w2):
        hbm = pl.BlockSpec(memory_space=pltpu.HBM)
        sem = pltpu.SemaphoreType.DMA
        steps = 2 * NCOL
        tok = jax.ShapeDtypeStruct((TOK, D), BF16)
        out = pl.pallas_call(
            kernel,
            name="moe_layer",
            out_shape=(tok, tok, jax.ShapeDtypeStruct((D, F), BF16), jax.ShapeDtypeStruct((D, F), BF16), jax.ShapeDtypeStruct((F, D), BF16)),
            in_specs=[hbm] * 14,
            out_specs=(hbm,) * 5,
            scratch_shapes=[
                pltpu.VMEM((NSRC, 2, 2, TOP_K, TOK), jnp.int32),
                pltpu.VMEM((NSRC, 2, TOP_K, TOK), F32),
                pltpu.VMEM((2, NSRC, TOK, D), BF16),
                pltpu.VMEM((2, NSRC, EXP, 1, TOK), jnp.int32),
                pltpu.VMEM((2, NSRC, TOK, 3 * EXP * CAP), BF16),
                pltpu.VMEM((GRP, ROWS, D), BF16),
                pltpu.VMEM((2 * TOK, F), BF16),
                pltpu.VMEM((EXP * SIDE, F), BF16),
                pltpu.VMEM((EXP * ROWS, F), BF16),
                pltpu.VMEM((NSRC, EXP, CAP, COL), BF16),
                pltpu.VMEM((2, TOK, COL), F32),
                pltpu.VMEM((2, TOK, COL), F32),
                pltpu.VMEM((steps, TOK, COL), F32),
                pltpu.VMEM((steps, TOK, COL), F32),
                pltpu.VMEM((steps, TOK, COL), F32),
                pltpu.VMEM((SLOTS13, 2, D, F), BF16),
                pltpu.VMEM((SLOTS2, HALF, F, COL), BF16),
                sem((2, 4)), sem((2, 2, 3)), sem((2, 2, 3)), sem((2, 3)), sem((2, 3)), sem((2,)), sem((2,)), sem((2, 2)), sem((2, 2)), sem((2, 2)), sem((2, 2)),
                sem((steps,)), sem((steps,)), sem((steps,)), sem((steps,)), sem((steps,)), sem((steps,)),
                sem((3,)), sem((3,)), sem((3,)), sem((3,)), sem((SLOTS13, 2)), sem((SLOTS2,)), sem((NCOL, 2)), sem((steps,)),
            ],
            compiler_params=pltpu.CompilerParams(collective_id=0, has_side_effects=True, vmem_limit_bytes=67043328),
        )(tokens_a, tokens_b, experts_a.T, experts_b.T, gates_a.T, gates_b.T, slots_a.T, slots_b.T,
          shared_w1, shared_w3, shared_w2, routed_w1, routed_w3, routed_w2)
        return tuple(pl.pallas_call(
            hand_over,
            name="hand_over",
            out_shape=(tok, tok),
            in_specs=[hbm] * 2,
            out_specs=(hbm,) * 2,
            scratch_shapes=[pltpu.VMEM((2, TOK, D), BF16), sem((2, 4)), sem((2, 4))],
        )(out[0], out[1]))

    return jax.shard_map(layer_local, mesh=mesh, in_specs=in_specs, out_specs=(tok_spec, tok_spec), check_vma=False)
```

```python
import functools

import jax
import jax.numpy as jnp
from jax import lax
from jax.experimental import pallas as pl
from jax.experimental.pallas import tpu as pltpu
from jax.sharding import PartitionSpec as P

MESH = pl.DeviceIdType.MESH
BF16 = jnp.bfloat16
F32 = jnp.float32

TOK = 256
D = 1280
F = 896
TOP_K = 6
CAP = 48
EXP = 16
NSRC = 4
XP, DG, OWN, CP = range(NSRC)
GRP = 4
COL = 256
NCOL = D // COL
ROWS = NSRC * CAP
SIDE = 2 * CAP
SLOTS13 = 4
SLOTS2 = 5
PER = 4
BLOCKS = EXP // PER


def dot(a, b):
    return jnp.dot(a, b, preferred_element_type=F32)


def kernel(xa, xb, ea, eb, ga, gb, sa, sb, sw1, sw3, sw2, rw1, rw3, rw2,
           oa, ob, pw1, pw3, pw2,
           ids, gates, tokbuf, slots, gmat, rowsg, hs, hfar, hnear, ybuf, work, q0, q2, rr, w13, w2b,
           own_s, meta_s, meta_r, fmeta_s, fmeta_r, tc_s, tc_r, tx_s, tx_r, td_s, td_r, p1_s, p1_r, p3_s, p3_r, rr_s, rr_r,
           yw_s, yw_r, fw_s, fw_r, w13_s, w2_s, sw2_s):
    ep = lax.axis_index("ep")
    tp = lax.axis_index("tp")
    core = lax.rem(ep, 2)
    core_peer = {"ep": ep + 1 - 2 * core}
    x_peer = {"ep": lax.rem(ep + 2, 4)}
    diag = {"ep": 3 - ep}
    y_peer = {"tp": 1 - tp}
    own = (xa, xb)

    def remote(src, dst, s, r, dev):
        return pltpu.make_async_remote_copy(src_ref=src, dst_ref=dst, send_sem=s, recv_sem=r, device_id=dev, device_id_type=MESH)

    def expert_of(u):
        return lax.rem(jnp.where(u < EXP, u, u + EXP - SLOTS13), EXP)

    def w13_copies(u):
        slot = lax.rem(u, SLOTS13)
        e = expert_of(u)
        return (pltpu.make_async_copy(rw1.at[e], w13.at[slot, 0], w13_s.at[slot, 0]),
                pltpu.make_async_copy(rw3.at[e], w13.at[slot, 1], w13_s.at[slot, 1]))

    def w2_copy(unit):
        slot = lax.rem(unit, SLOTS2)
        n = lax.rem(lax.div(unit, BLOCKS), NCOL)
        first = lax.rem(unit, BLOCKS) * PER
        return pltpu.make_async_copy(rw2.at[pl.ds(first, PER), :, pl.ds(pl.multiple_of(n * COL, COL), COL)], w2b.at[slot], w2_s.at[slot])

    routing = ((ea, sa, ga), (eb, sb, gb))

    def routing_slots(m, src):
        return ids.at[src, m, 0], ids.at[src, m, 1], gates.at[src, m]

    own_cp = [pltpu.make_async_copy(a, b, own_s.at[m, k]) for m in range(2)
              for k, (a, b) in enumerate(zip((*routing[m], own[m]), (*routing_slots(m, OWN), tokbuf.at[m, OWN])))]
    for cp in own_cp:
        cp.start()

    barrier = pltpu.get_barrier_semaphore()
    for dev in (core_peer, x_peer, diag, y_peer):
        pl.semaphore_signal(barrier, inc=1, device_id=dev, device_id_type=MESH)
    pl.semaphore_wait(barrier, 4)

    def routing_cp(m, k, src, dst, ss, rs, dev):
        return remote(src[k], routing_slots(m, dst)[k], ss.at[m, k], rs.at[m, k], dev)

    cmeta_cp = [[routing_cp(m, k, routing[m], CP, meta_s.at[0], meta_r.at[0], core_peer) for k in range(3)] for m in range(2)]
    xmeta_cp = [[routing_cp(m, k, routing[m], XP, meta_s.at[1], meta_r.at[1], x_peer) for k in range(3)] for m in range(2)]
    dmeta_cp = [[routing_cp(m, k, routing_slots(m, XP), DG, fmeta_s, fmeta_r, core_peer) for k in range(3)] for m in range(2)]
    part = TOK // 2
    x_cp = [[remote(own[m].at[pl.ds(k * part, part)], tokbuf.at[m, XP, pl.ds(k * part, part)], tx_s.at[m, k], tx_r.at[m, k], x_peer) for k in range(2)] for m in range(2)]
    d_cp = [[remote(tokbuf.at[m, XP, pl.ds(k * part, part)], tokbuf.at[m, DG, pl.ds(k * part, part)], td_s.at[m, k], td_r.at[m, k], core_peer) for k in range(2)] for m in range(2)]
    c_cp = [remote(own[m], tokbuf.at[m, CP], tc_s.at[m], tc_r.at[m], core_peer) for m in range(2)]
    for cp in (*xmeta_cp[0], *xmeta_cp[1], *cmeta_cp[0], *cmeta_cp[1], *x_cp[0], *c_cp):
        cp.start()
    local13 = (pltpu.make_async_copy(sw1, w13.at[SLOTS13 - 1, 0], w13_s.at[SLOTS13 - 1, 0]),
               pltpu.make_async_copy(sw3, w13.at[SLOTS13 - 1, 1], w13_s.at[SLOTS13 - 1, 1]))
    for cp in local13:
        cp.start()
    for u in range(SLOTS13 - 1):
        for cp in w13_copies(jnp.int32(u)):
            cp.start()

    half_d, half_f = D // 2, F // 2
    rows_d = pl.ds(pl.multiple_of(core * half_d, 128), half_d)
    rows_f = pl.ds(pl.multiple_of(core * half_f, 64), half_f)
    yw_cp = [remote(w.at[r], p.at[r], yw_s.at[i], yw_r.at[i], y_peer)
             for i, (w, p, r) in enumerate(((sw1, pw1, rows_d), (sw3, pw3, rows_d), (sw2, pw2, rows_f)))]
    fw_cp = [remote(p.at[r], p.at[r], fw_s.at[i], fw_r.at[i], core_peer)
             for i, (p, r) in enumerate(((pw1, rows_d), (pw3, rows_d), (pw2, rows_f)))]
    for cp in yw_cp:
        cp.start()
    for unit in range(SLOTS2):
        w2_copy(jnp.int32(unit)).start()

    for cp in own_cp:
        cp.wait()

    def route(i, carry):
        m, src = carry, i
        first = ep * EXP + lax.broadcasted_iota(jnp.int32, (EXP, TOK), 0)
        id_rows, slot_rows, gate_rows = ids[src, m, 0], ids[src, m, 1], gates[src, m]
        slot = jnp.full((EXP, TOK), -1, jnp.int32)
        gate = jnp.zeros((EXP, TOK), F32)
        for j in range(TOP_K):
            hit = (id_rows[j:j + 1, :] == first) & (slot_rows[j:j + 1, :] >= 0)
            slot = jnp.where(hit, slot_rows[j:j + 1, :], slot)
            gate = jnp.where(hit, gate_rows[j:j + 1, :], gate)
        pos = lax.broadcasted_iota(jnp.int32, (CAP, TOK), 0)
        for e in range(EXP):
            slots[m, src, e] = slot[e:e + 1, :]
        part = EXP // 2
        for k in range(2):
            g = jnp.concatenate([jnp.where(pos == slot[e:e + 1, :], gate[e:e + 1, :], 0.0)
                                 for e in range(k * part, (k + 1) * part)], axis=0).T
            hi = g.astype(BF16)
            g = g - hi.astype(F32)
            mid = g.astype(BF16)
            low = (g - mid.astype(F32)).astype(BF16)
            for p, v in enumerate((hi, mid, low)):
                gmat[m, src, :, pl.ds(p * EXP * CAP + k * part * CAP, part * CAP)] = v
        return carry

    def route_all(m):
        for cp in (*xmeta_cp[m], *cmeta_cp[m]):
            cp.wait()
        for cp in dmeta_cp[m]:
            cp.start()
        for cp in dmeta_cp[m]:
            cp.wait()
        lax.fori_loop(0, NSRC, route, jnp.int32(m))

    def arrive(m):
        for k in range(2):
            x_cp[m][k].wait()
            d_cp[m][k].start()

    def swiglu_in(x, w1, w3, store):
        full = F // COL
        for k in range(full):
            cols = pl.ds(k * COL, COL)
            a = dot(x, w1[:, cols])
            b = dot(x, w3[:, cols])
            store(cols, (jax.nn.silu(a) * b).astype(BF16))
        cols = pl.ds(full * COL, F - full * COL)
        ab = dot(x, jnp.concatenate([w1[:, cols], w3[:, cols]], axis=1))
        a, b = ab[:, :F - full * COL], ab[:, F - full * COL:]
        store(cols, (jax.nn.silu(a) * b).astype(BF16))

    def gather(g, places):
        pos = lax.broadcasted_iota(jnp.int32, (CAP, TOK), 0)
        for k, (m, src) in enumerate(places):
            place = jnp.concatenate([jnp.where(pos == slots[m, src, g * GRP + i], 1.0, 0.0) for i in range(GRP)], axis=0).astype(BF16)
            for n in range(NCOL):
                cols = pl.ds(n * COL, COL)
                r = dot(place, tokbuf[m, src, :, cols]).astype(BF16)
                for i in range(GRP):
                    rowsg[i, pl.ds(k * CAP, CAP), cols] = r[i * CAP:(i + 1) * CAP]

    def early():
        gather(0, [(m, src) for m in range(2) for src in (OWN, CP)])

        def expert(i, carry):
            for cp in w13_copies(i):
                cp.wait()
            rows = pl.ds(pl.multiple_of(i * ROWS, ROWS), ROWS)

            def store(cols, v):
                hnear[rows, cols] = v

            swiglu_in(rowsg[i], w13.at[i, 0], w13.at[i, 1], store)
            return carry

        lax.fori_loop(0, GRP, expert, 0)

    def phase1(m, after_gather):
        def run(t, g, all_rows):
            gather(g, [(m, src) for src in ((XP, DG, OWN, CP) if all_rows else (XP, DG))])
            after_gather(t)

            def expert(i, carry):
                u = m * EXP + t * GRP + i
                slot = lax.rem(u, SLOTS13)
                rows = pl.ds(pl.multiple_of((g * GRP + i) * SIDE, SIDE), SIDE)
                near = pl.ds(pl.multiple_of((g * GRP + i) * ROWS + m * SIDE, SIDE), SIDE)

                @pl.when((u >= SLOTS13) & ((u < EXP) | (u >= EXP + SLOTS13)))
                def _():
                    for cp in w13_copies(u):
                        cp.wait()

                def store(cols, v):
                    hfar[rows, cols] = v[:SIDE]
                    if all_rows:
                        hnear[near, cols] = v[SIDE:]

                swiglu_in(rowsg[i] if all_rows else rowsg[i, :SIDE], w13.at[slot, 0], w13.at[slot, 1], store)
                nxt = u + SLOTS13

                @pl.when((nxt < EXP) | ((nxt >= EXP + SLOTS13) & (nxt < 2 * EXP)))
                def _():
                    for cp in w13_copies(nxt):
                        cp.start()
                return carry

            lax.fori_loop(0, GRP, expert, 0)

        def group(t, carry):
            g = lax.rem(t + m * (EXP // GRP - 1), EXP // GRP)

            @pl.when(g == 0)
            def _():
                run(t, g, False)

            @pl.when(g > 0)
            def _():
                run(t, g, True)
            return carry

        lax.fori_loop(0, EXP // GRP, group, 0)

    def expand(step, h, sources, blocks=range(BLOCKS), refills=BLOCKS):
        size = sources * CAP
        for b in blocks:
            w2_copy(step * BLOCKS + b).wait()
        for b in blocks:
            slot = lax.rem(step * BLOCKS + b, SLOTS2)
            for i in range(PER):
                e = b * PER + i
                y = dot(h[e * size:(e + 1) * size, :], w2b[slot, i]).astype(BF16)
                for k in range(sources):
                    ybuf[k, e] = y[k * CAP:(k + 1) * CAP]
            if b < refills:
                w2_copy(step * BLOCKS + b + SLOTS2).start()

    def combine(k, m, src):
        y = ybuf[k].reshape(EXP * CAP, COL)
        n = EXP * CAP
        g = gmat.at[m, src]
        return dot(g[:, :n], y) + dot(g[:, n:2 * n], y) + dot(g[:, 2 * n:], y)

    def far_copies(step):
        par = lax.rem(step, 2)
        return (remote(work.at[par], q2.at[step], p3_s.at[step], p3_r.at[step], core_peer),
                remote(q2.at[step], rr.at[step], rr_s.at[step], rr_r.at[step], x_peer))

    def near_copy(m, n):
        return remote(work.at[2 * lax.rem(n, 2) + m], q0.at[m * NCOL + n], p1_s.at[m * NCOL + n], p1_r.at[m * NCOL + n], core_peer)

    def finish(step):
        cp, back = far_copies(step)
        cp.wait()
        q2[step] = q2[step] + work[2 + lax.rem(step, 2)]
        back.start()

    def far(m, during):
        def column(n, carry):
            step = m * NCOL + n
            expand(step, hfar, 2, range(BLOCKS // 2))

            @pl.when(n == 1)
            def _():
                finish(step - 1)

            expand(step, hfar, 2, range(BLOCKS // 2, BLOCKS))
            par = lax.rem(step, 2)
            work[par] = combine(DG, m, DG)
            work[2 + par] = combine(XP, m, XP)
            far_copies(step)[0].start()

            during(n)

            @pl.when(n >= 2)
            def _():
                finish(step - 1)
            return carry

        lax.fori_loop(0, NCOL, column, 0)

    def shared_in(half, slot):
        for m in range(2):
            def store(cols, v):
                hs_of(half, m)[:, cols] = v

            swiglu_in(tokbuf[m, OWN], w13.at[slot, 0], w13.at[slot, 1], store)

    def hs_of(half, m):
        rows = pl.ds(m * TOK, TOK)
        return hfar.at[rows, :] if half else hs.at[rows, :]

    for cp in local13:
        cp.wait()
    shared_in(0, SLOTS13 - 1)
    for cp in w13_copies(jnp.int32(SLOTS13 - 1)):
        cp.start()
    route_all(0)
    route_all(1)
    for cp in c_cp:
        cp.wait()
    early()
    arrive(0)
    for cp in x_cp[1]:
        cp.start()
    for cp in d_cp[0]:
        cp.wait()
    phase1(0, lambda t: None)
    arrive(1)
    far(0, lambda n: None)
    for cp in d_cp[1]:
        cp.wait()

    def between(t):
        @pl.when(t == 1)
        def _():
            finish(jnp.int32(NCOL - 1))

        @pl.when(t == 2)
        def _():
            for i in range(2):
                yw_cp[i].wait()
                fw_cp[i].start()

    phase1(1, between)

    peer13 = (pltpu.make_async_copy(pw1, w13.at[1, 0], w13_s.at[1, 0]), pltpu.make_async_copy(pw3, w13.at[1, 1], w13_s.at[1, 1]))

    def sw2_slot(half, n):
        return w13.at[2 + half, lax.div(n, 3), pl.ds(0, F), pl.ds(pl.multiple_of(lax.rem(n, 3) * COL, COL), COL)]

    def sw2_copy(half, n):
        return pltpu.make_async_copy((sw2, pw2)[half].at[:, pl.ds(pl.multiple_of(n * COL, COL), COL)], sw2_slot(half, n), sw2_s.at[n, half])


    def fetch_peer(n):
        for i in range(2):
            @pl.when(n == 2 + i)
            def _():
                fw_cp[i].wait()
                peer13[i].start()

        @pl.when(n == 3)
        def _():
            yw_cp[2].wait()
            fw_cp[2].start()

    far(1, fetch_peer)
    for n in range(NCOL):
        sw2_copy(0, jnp.int32(n)).start()
    fw_cp[2].wait()
    for n in range(NCOL):
        sw2_copy(1, jnp.int32(n)).start()
    for cp in peer13:
        cp.wait()
    shared_in(1, 1)
    finish(jnp.int32(2 * NCOL - 1))

    def near_finish(n):
        for m in range(2):
            step = m * NCOL + n
            near_copy(m, n).wait()
            back = far_copies(step)[1]
            back.wait_recv()
            if m:
                back.wait_send()
            mine = q2[2 * lax.rem(n, 2) + m]
            (oa, ob)[m][:, pl.ds(pl.multiple_of(n * COL, COL), COL)] = (q0[step] + rr[step] + mine).astype(BF16)

    for n in range(NCOL):
        far_copies(jnp.int32(n))[1].wait_send()

    def near_column(n, carry, refills=BLOCKS, final=False):
        for half in range(2):
            sw2_copy(half, n).wait()
        expand(2 * NCOL + n, hnear, NSRC, refills=refills)
        base = 2 * lax.rem(n, 2)
        cols = pl.ds(pl.multiple_of(n * COL, COL), COL)
        for m in range(2):
            work[base + m] = combine(2 * m + 1, m, CP)
        if final:
            for m in range(2):
                near_copy(m, n).start()
        for m in range(2):
            s = dot(hs_of(0, m)[...], sw2_slot(0, n)[...]) + dot(hs_of(1, m)[...], sw2_slot(1, n)[...])
            q2[base + m] = s + tokbuf[m, OWN, :, cols].astype(F32) + combine(2 * m, m, OWN)
        if not final:
            for m in range(2):
                near_copy(m, n).start()

        @pl.when(n >= 1)
        def _():
            near_finish(n - 1)
        return carry

    last = NCOL * BLOCKS * 3 - SLOTS2
    full = (last - 2 * NCOL * BLOCKS) // BLOCKS
    lax.fori_loop(0, full, near_column, 0)
    for n in range(full, NCOL):
        near_column(jnp.int32(n), 0, max(0, last - (2 * NCOL + n) * BLOCKS), n == NCOL - 1)
    near_finish(jnp.int32(NCOL - 1))


def solution(mesh):
    tok_spec = P(('data', 'ep', 'tp'), None)
    in_specs = (tok_spec,) * 8 + (P(None, 'tp'), P(None, 'tp'), P('tp', None), P('ep', None, None), P('ep', None, None), P('ep', None, None))

    def layer_local(tokens_a, tokens_b, experts_a, experts_b, gates_a, gates_b, slots_a, slots_b,
                    shared_w1, shared_w3, shared_w2, routed_w1, routed_w3, routed_w2):
        hbm = pl.BlockSpec(memory_space=pltpu.HBM)
        vmem = pl.BlockSpec(memory_space=pltpu.VMEM)
        sem = pltpu.SemaphoreType.DMA
        steps = 2 * NCOL
        tok = jax.ShapeDtypeStruct((TOK, D), BF16)
        out = pl.pallas_call(
            kernel,
            name="moe_layer",
            out_shape=(pltpu.VMEM((TOK, D), BF16), pltpu.VMEM((TOK, D), BF16), jax.ShapeDtypeStruct((D, F), BF16), jax.ShapeDtypeStruct((D, F), BF16), jax.ShapeDtypeStruct((F, D), BF16)),
            in_specs=[hbm] * 14,
            out_specs=(vmem,) * 2 + (hbm,) * 3,
            scratch_shapes=[
                pltpu.VMEM((NSRC, 2, 2, TOP_K, TOK), jnp.int32),
                pltpu.VMEM((NSRC, 2, TOP_K, TOK), F32),
                pltpu.VMEM((2, NSRC, TOK, D), BF16),
                pltpu.VMEM((2, NSRC, EXP, 1, TOK), jnp.int32),
                pltpu.VMEM((2, NSRC, TOK, 3 * EXP * CAP), BF16),
                pltpu.VMEM((GRP, ROWS, D), BF16),
                pltpu.VMEM((2 * TOK, F), BF16),
                pltpu.VMEM((EXP * SIDE, F), BF16),
                pltpu.VMEM((EXP * ROWS, F), BF16),
                pltpu.VMEM((NSRC, EXP, CAP, COL), BF16),
                pltpu.VMEM((4, TOK, COL), F32),
                pltpu.VMEM((steps, TOK, COL), F32),
                pltpu.VMEM((steps, TOK, COL), F32),
                pltpu.VMEM((steps, TOK, COL), F32),
                pltpu.VMEM((SLOTS13, 2, D, F), BF16),
                pltpu.VMEM((SLOTS2, PER, F, COL), BF16),
                sem((2, 4)), sem((2, 2, 3)), sem((2, 2, 3)), sem((2, 3)), sem((2, 3)), sem((2,)), sem((2,)), sem((2, 2)), sem((2, 2)), sem((2, 2)), sem((2, 2)),
                sem((steps,)), sem((steps,)), sem((steps,)), sem((steps,)), sem((steps,)), sem((steps,)),
                sem((3,)), sem((3,)), sem((3,)), sem((3,)), sem((SLOTS13, 2)), sem((SLOTS2,)), sem((NCOL, 2)),
            ],
            compiler_params=pltpu.CompilerParams(collective_id=0, has_side_effects=True, vmem_limit_bytes=67043328 - 1376256),
        )(tokens_a, tokens_b, experts_a.T, experts_b.T, gates_a.T, gates_b.T, slots_a.T, slots_b.T,
          shared_w1, shared_w3, shared_w2, routed_w1, routed_w3, routed_w2)
        return out[0], out[1]

    return jax.shard_map(layer_local, mesh=mesh, in_specs=in_specs, out_specs=(tok_spec, tok_spec), check_vma=False)
```

```python
import functools

import jax
import jax.numpy as jnp
from jax import lax
from jax.experimental import pallas as pl
from jax.experimental.pallas import tpu as pltpu
from jax.sharding import PartitionSpec as P

MESH = pl.DeviceIdType.MESH
BF16 = jnp.bfloat16
F32 = jnp.float32

TOK = 256
D = 1280
F = 896
TOP_K = 6
CAP = 48
EXP = 16
NSRC = 4
XP, DG, OWN, CP = range(NSRC)
GRP = 4
COL = 256
NCOL = D // COL
ROWS = NSRC * CAP
SIDE = 2 * CAP
SLOTS13 = 4
SLOTS2 = 5
PER = 4
BLOCKS = EXP // PER


def dot(a, b):
    return jnp.dot(a, b, preferred_element_type=F32)


def kernel(xa, xb, ea, eb, ga, gb, sa, sb, sw1, sw3, sw2, rw1, rw3, rw2,
           oa, ob, pw1, pw3, pw2,
           ids, gates, tokbuf, slots, gmat, rowsg, hs, hfar, hnear, ybuf, work, q0, q2, rr, w13, w2b,
           own_s, meta_s, meta_r, fmeta_s, fmeta_r, tc_s, tc_r, tx_s, tx_r, td_s, td_r, p1_s, p1_r, p3_s, p3_r, rr_s, rr_r,
           yw_s, yw_r, fw_s, fw_r, w13_s, w2_s, sw2_s):
    ep = lax.axis_index("ep")
    tp = lax.axis_index("tp")
    core = lax.rem(ep, 2)
    core_peer = {"ep": ep + 1 - 2 * core}
    x_peer = {"ep": lax.rem(ep + 2, 4)}
    diag = {"ep": 3 - ep}
    y_peer = {"tp": 1 - tp}
    own = (xa, xb)

    def remote(src, dst, s, r, dev):
        return pltpu.make_async_remote_copy(src_ref=src, dst_ref=dst, send_sem=s, recv_sem=r, device_id=dev, device_id_type=MESH)

    def expert_of(u):
        return lax.rem(jnp.where(u < EXP, u, u + EXP - SLOTS13), EXP)

    def w13_copies(u):
        slot = lax.rem(u, SLOTS13)
        e = expert_of(u)
        return (pltpu.make_async_copy(rw1.at[e], w13.at[slot, 0], w13_s.at[slot, 0]),
                pltpu.make_async_copy(rw3.at[e], w13.at[slot, 1], w13_s.at[slot, 1]))

    def w2_copy(unit):
        slot = lax.rem(unit, SLOTS2)
        n = lax.rem(lax.div(unit, BLOCKS), NCOL)
        first = lax.rem(unit, BLOCKS) * PER
        return pltpu.make_async_copy(rw2.at[pl.ds(first, PER), :, pl.ds(pl.multiple_of(n * COL, COL), COL)], w2b.at[slot], w2_s.at[slot])

    routing = ((ea, sa, ga), (eb, sb, gb))

    def routing_slots(m, src):
        return ids.at[src, m, 0], ids.at[src, m, 1], gates.at[src, m]

    own_cp = [pltpu.make_async_copy(a, b, own_s.at[m, k]) for m in range(2)
              for k, (a, b) in enumerate(zip((*routing[m], own[m]), (*routing_slots(m, OWN), tokbuf.at[m, OWN])))]
    for cp in own_cp:
        cp.start()

    barrier = pltpu.get_barrier_semaphore()
    for dev in (core_peer, x_peer, diag, y_peer):
        pl.semaphore_signal(barrier, inc=1, device_id=dev, device_id_type=MESH)
    pl.semaphore_wait(barrier, 4)

    def routing_cp(m, k, src, dst, ss, rs, dev):
        return remote(src[k], routing_slots(m, dst)[k], ss.at[m, k], rs.at[m, k], dev)

    cmeta_cp = [[routing_cp(m, k, routing[m], CP, meta_s.at[0], meta_r.at[0], core_peer) for k in range(3)] for m in range(2)]
    xmeta_cp = [[routing_cp(m, k, routing[m], XP, meta_s.at[1], meta_r.at[1], x_peer) for k in range(3)] for m in range(2)]
    dmeta_cp = [[routing_cp(m, k, routing_slots(m, XP), DG, fmeta_s, fmeta_r, core_peer) for k in range(3)] for m in range(2)]
    part = TOK // 2
    x_cp = [[remote(own[m].at[pl.ds(k * part, part)], tokbuf.at[m, XP, pl.ds(k * part, part)], tx_s.at[m, k], tx_r.at[m, k], x_peer) for k in range(2)] for m in range(2)]
    d_cp = [[remote(tokbuf.at[m, XP, pl.ds(k * part, part)], tokbuf.at[m, DG, pl.ds(k * part, part)], td_s.at[m, k], td_r.at[m, k], core_peer) for k in range(2)] for m in range(2)]
    c_cp = [remote(own[m], tokbuf.at[m, CP], tc_s.at[m], tc_r.at[m], core_peer) for m in range(2)]
    for cp in (*xmeta_cp[0], *xmeta_cp[1], *cmeta_cp[0], *cmeta_cp[1], *x_cp[0], *c_cp):
        cp.start()
    local13 = (pltpu.make_async_copy(sw1, w13.at[SLOTS13 - 1, 0], w13_s.at[SLOTS13 - 1, 0]),
               pltpu.make_async_copy(sw3, w13.at[SLOTS13 - 1, 1], w13_s.at[SLOTS13 - 1, 1]))
    for cp in local13:
        cp.start()
    for u in range(SLOTS13 - 1):
        for cp in w13_copies(jnp.int32(u)):
            cp.start()

    half_d, half_f = D // 2, F // 2
    rows_d = pl.ds(pl.multiple_of(core * half_d, 128), half_d)
    rows_f = pl.ds(pl.multiple_of(core * half_f, 64), half_f)
    yw_cp = [remote(w.at[r], p.at[r], yw_s.at[i], yw_r.at[i], y_peer)
             for i, (w, p, r) in enumerate(((sw1, pw1, rows_d), (sw3, pw3, rows_d), (sw2, pw2, rows_f)))]
    fw_cp = [remote(p.at[r], p.at[r], fw_s.at[i], fw_r.at[i], core_peer)
             for i, (p, r) in enumerate(((pw1, rows_d), (pw3, rows_d), (pw2, rows_f)))]
    for cp in yw_cp:
        cp.start()
    for unit in range(SLOTS2):
        w2_copy(jnp.int32(unit)).start()

    for cp in own_cp:
        cp.wait()

    def route(i, carry):
        m, src = carry, i
        first = ep * EXP + lax.broadcasted_iota(jnp.int32, (EXP, TOK), 0)
        id_rows, slot_rows, gate_rows = ids[src, m, 0], ids[src, m, 1], gates[src, m]
        slot = jnp.full((EXP, TOK), -1, jnp.int32)
        gate = jnp.zeros((EXP, TOK), F32)
        for j in range(TOP_K):
            hit = (id_rows[j:j + 1, :] == first) & (slot_rows[j:j + 1, :] >= 0)
            slot = jnp.where(hit, slot_rows[j:j + 1, :], slot)
            gate = jnp.where(hit, gate_rows[j:j + 1, :], gate)
        pos = lax.broadcasted_iota(jnp.int32, (CAP, TOK), 0)
        for e in range(EXP):
            slots[m, src, e] = slot[e:e + 1, :]
        part = EXP // 2
        for k in range(2):
            g = jnp.concatenate([jnp.where(pos == slot[e:e + 1, :], gate[e:e + 1, :], 0.0)
                                 for e in range(k * part, (k + 1) * part)], axis=0).T
            hi = g.astype(BF16)
            g = g - hi.astype(F32)
            mid = g.astype(BF16)
            low = (g - mid.astype(F32)).astype(BF16)
            for p, v in enumerate((hi, mid, low)):
                gmat[m, src, :, pl.ds(p * EXP * CAP + k * part * CAP, part * CAP)] = v
        return carry

    def route_all(m):
        for cp in (*xmeta_cp[m], *cmeta_cp[m]):
            cp.wait()
        for cp in dmeta_cp[m]:
            cp.start()
        for cp in dmeta_cp[m]:
            cp.wait()
        lax.fori_loop(0, NSRC, route, jnp.int32(m))

    def arrive(m):
        for k in range(2):
            x_cp[m][k].wait()
            d_cp[m][k].start()

    def swiglu_in(x, w1, w3, store):
        full = F // COL
        for k in range(full):
            cols = pl.ds(k * COL, COL)
            a = dot(x, w1[:, cols])
            b = dot(x, w3[:, cols])
            store(cols, (jax.nn.silu(a) * b).astype(BF16))
        cols = pl.ds(full * COL, F - full * COL)
        ab = dot(x, jnp.concatenate([w1[:, cols], w3[:, cols]], axis=1))
        a, b = ab[:, :F - full * COL], ab[:, F - full * COL:]
        store(cols, (jax.nn.silu(a) * b).astype(BF16))

    def gather(g, places):
        pos = lax.broadcasted_iota(jnp.int32, (CAP, TOK), 0)
        for k, (m, src) in enumerate(places):
            place = jnp.concatenate([jnp.where(pos == slots[m, src, g * GRP + i], 1.0, 0.0) for i in range(GRP)], axis=0).astype(BF16)
            for n in range(NCOL):
                cols = pl.ds(n * COL, COL)
                r = dot(place, tokbuf[m, src, :, cols]).astype(BF16)
                for i in range(GRP):
                    rowsg[i, pl.ds(k * CAP, CAP), cols] = r[i * CAP:(i + 1) * CAP]

    def early():
        gather(0, [(m, src) for m in range(2) for src in (OWN, CP)])

        def expert(i, carry):
            for cp in w13_copies(i):
                cp.wait()
            rows = pl.ds(pl.multiple_of(i * ROWS, ROWS), ROWS)

            def store(cols, v):
                hnear[rows, cols] = v

            swiglu_in(rowsg[i], w13.at[i, 0], w13.at[i, 1], store)
            return carry

        lax.fori_loop(0, GRP, expert, 0)

    def phase1(m, after_gather):
        def run(t, g, all_rows):
            gather(g, [(m, src) for src in ((XP, DG, OWN, CP) if all_rows else (XP, DG))])
            after_gather(t)

            def expert(i, carry):
                u = m * EXP + t * GRP + i
                slot = lax.rem(u, SLOTS13)
                rows = pl.ds(pl.multiple_of((g * GRP + i) * SIDE, SIDE), SIDE)
                near = pl.ds(pl.multiple_of((g * GRP + i) * ROWS + m * SIDE, SIDE), SIDE)

                @pl.when((u >= SLOTS13) & ((u < EXP) | (u >= EXP + SLOTS13)))
                def _():
                    for cp in w13_copies(u):
                        cp.wait()

                def store(cols, v):
                    hfar[rows, cols] = v[:SIDE]
                    if all_rows:
                        hnear[near, cols] = v[SIDE:]

                swiglu_in(rowsg[i] if all_rows else rowsg[i, :SIDE], w13.at[slot, 0], w13.at[slot, 1], store)
                nxt = u + SLOTS13

                @pl.when((nxt < EXP) | ((nxt >= EXP + SLOTS13) & (nxt < 2 * EXP)))
                def _():
                    for cp in w13_copies(nxt):
                        cp.start()
                return carry

            lax.fori_loop(0, GRP, expert, 0)

        def group(t, carry):
            g = lax.rem(t + m * (EXP // GRP - 1), EXP // GRP)

            @pl.when(g == 0)
            def _():
                run(t, g, False)

            @pl.when(g > 0)
            def _():
                run(t, g, True)
            return carry

        lax.fori_loop(0, EXP // GRP, group, 0)

    def expand(step, h, sources, blocks=range(BLOCKS), refills=BLOCKS):
        size = sources * CAP
        for b in blocks:
            w2_copy(step * BLOCKS + b).wait()
        for b in blocks:
            slot = lax.rem(step * BLOCKS + b, SLOTS2)
            for i in range(PER):
                e = b * PER + i
                y = dot(h[e * size:(e + 1) * size, :], w2b[slot, i]).astype(BF16)
                for k in range(sources):
                    ybuf[k, e] = y[k * CAP:(k + 1) * CAP]
            if b < refills:
                w2_copy(step * BLOCKS + b + SLOTS2).start()

    def combine(k, m, src):
        y = ybuf[k].reshape(EXP * CAP, COL)
        n = EXP * CAP
        g = gmat.at[m, src]
        return dot(g[:, :n], y) + dot(g[:, n:2 * n], y) + dot(g[:, 2 * n:], y)

    def far_copies(step):
        par = lax.rem(step, 2)
        return (remote(work.at[par], q2.at[step], p3_s.at[par], p3_r.at[step], core_peer),
                remote(q2.at[step], rr.at[step], rr_s.at[step], rr_r.at[step], x_peer))

    def near_copy(m, n):
        return remote(work.at[2 * lax.rem(n, 2) + m], q0.at[m * NCOL + n], p1_s.at[2 * lax.rem(n, 2) + m], p1_r.at[m * NCOL + n], core_peer)

    def finish(step):
        cp, back = far_copies(step)
        cp.wait()
        q2[step] = q2[step] + work[2 + lax.rem(step, 2)]
        back.start()

    def far(m, during):
        def column(n, carry):
            step = m * NCOL + n
            expand(step, hfar, 2, range(BLOCKS // 2))

            if m:
                @pl.when(n == 1)
                def _():
                    finish(step - 1)

            expand(step, hfar, 2, range(BLOCKS // 2, BLOCKS))
            par = lax.rem(step, 2)
            work[par] = combine(DG, m, DG)
            work[2 + par] = combine(XP, m, XP)
            far_copies(step)[0].start()

            during(n)

            @pl.when(n >= 1 + m)
            def _():
                finish(step - 1)
            return carry

        lax.fori_loop(0, NCOL, column, 0)

    def shared_in(half, slot):
        for m in range(2):
            def store(cols, v):
                hs_of(half, m)[:, cols] = v

            swiglu_in(tokbuf[m, OWN], w13.at[slot, 0], w13.at[slot, 1], store)

    def hs_of(half, m):
        rows = pl.ds(m * TOK, TOK)
        return hfar.at[rows, :] if half else hs.at[rows, :]

    for cp in local13:
        cp.wait()
    shared_in(0, SLOTS13 - 1)
    for cp in w13_copies(jnp.int32(SLOTS13 - 1)):
        cp.start()
    route_all(0)
    route_all(1)
    for cp in c_cp:
        cp.wait()
    early()
    arrive(0)
    for cp in x_cp[1]:
        cp.start()
    for cp in d_cp[0]:
        cp.wait()
    phase1(0, lambda t: None)
    arrive(1)
    far(0, lambda n: None)
    for cp in d_cp[1]:
        cp.wait()

    def between(t):
        @pl.when(t == 1)
        def _():
            finish(jnp.int32(NCOL - 1))

        @pl.when(t == 2)
        def _():
            for i in range(2):
                yw_cp[i].wait()
                fw_cp[i].start()

    phase1(1, between)

    peer13 = (pltpu.make_async_copy(pw1, w13.at[1, 0], w13_s.at[1, 0]), pltpu.make_async_copy(pw3, w13.at[1, 1], w13_s.at[1, 1]))

    def sw2_slot(half, n):
        return w13.at[2 + half, lax.div(n, 3), pl.ds(0, F), pl.ds(pl.multiple_of(lax.rem(n, 3) * COL, COL), COL)]

    def sw2_copy(half, n):
        return pltpu.make_async_copy((sw2, pw2)[half].at[:, pl.ds(pl.multiple_of(n * COL, COL), COL)], sw2_slot(half, n), sw2_s.at[n, half])


    def fetch_peer(n):
        for i in range(2):
            @pl.when(n == 2 + i)
            def _():
                fw_cp[i].wait()
                peer13[i].start()

        @pl.when(n == 3)
        def _():
            yw_cp[2].wait()
            fw_cp[2].start()

    far(1, fetch_peer)
    for n in range(NCOL):
        sw2_copy(0, jnp.int32(n)).start()
    fw_cp[2].wait()
    for n in range(NCOL):
        sw2_copy(1, jnp.int32(n)).start()
    for cp in peer13:
        cp.wait()
    shared_in(1, 1)
    finish(jnp.int32(2 * NCOL - 1))

    def near_finish(n):
        for m in range(2):
            step = m * NCOL + n
            near_copy(m, n).wait()
            back = far_copies(step)[1]
            back.wait_recv()
            if m:
                back.wait_send()
            mine = q2[2 * lax.rem(n, 2) + m]
            (oa, ob)[m][:, pl.ds(pl.multiple_of(n * COL, COL), COL)] = (q0[step] + rr[step] + mine).astype(BF16)

    for n in range(NCOL):
        far_copies(jnp.int32(n))[1].wait_send()

    def near_column(n, carry, refills=BLOCKS, final=False):
        for half in range(2):
            sw2_copy(half, n).wait()
        expand(2 * NCOL + n, hnear, NSRC, refills=refills)
        base = 2 * lax.rem(n, 2)
        cols = pl.ds(pl.multiple_of(n * COL, COL), COL)
        for m in range(2):
            work[base + m] = combine(2 * m + 1, m, CP)
        if final:
            for m in range(2):
                near_copy(m, n).start()
        for m in range(2):
            s = dot(jnp.concatenate([hs_of(half, m)[...] for half in range(2)], axis=1),
                    jnp.concatenate([sw2_slot(half, n)[...] for half in range(2)], axis=0))
            q2[base + m] = s + tokbuf[m, OWN, :, cols].astype(F32) + combine(2 * m, m, OWN)
        if not final:
            for m in range(2):
                near_copy(m, n).start()

        @pl.when(n >= 1)
        def _():
            near_finish(n - 1)
        return carry

    last = NCOL * BLOCKS * 3 - SLOTS2
    full = (last - 2 * NCOL * BLOCKS) // BLOCKS
    lax.fori_loop(0, full, near_column, 0)
    for n in range(full, NCOL):
        near_column(jnp.int32(n), 0, max(0, last - (2 * NCOL + n) * BLOCKS), n == NCOL - 1)
    near_finish(jnp.int32(NCOL - 1))


def hand_over(a, b, oa, ob, out_s):
    copies = [pltpu.make_async_copy(src, dst, out_s.at[m]) for m, (src, dst) in enumerate(((a, oa), (b, ob)))]
    for cp in copies:
        cp.start()
    for cp in copies:
        cp.wait()


def solution(mesh):
    tok_spec = P(('data', 'ep', 'tp'), None)
    in_specs = (tok_spec,) * 8 + (P(None, 'tp'), P(None, 'tp'), P('tp', None), P('ep', None, None), P('ep', None, None), P('ep', None, None))

    def layer_local(tokens_a, tokens_b, experts_a, experts_b, gates_a, gates_b, slots_a, slots_b,
                    shared_w1, shared_w3, shared_w2, routed_w1, routed_w3, routed_w2):
        hbm = pl.BlockSpec(memory_space=pltpu.HBM)
        vmem = pl.BlockSpec(memory_space=pltpu.VMEM)
        sem = pltpu.SemaphoreType.DMA
        steps = 2 * NCOL
        tok = jax.ShapeDtypeStruct((TOK, D), BF16)
        out = pl.pallas_call(
            kernel,
            name="moe_layer",
            out_shape=(pltpu.VMEM((TOK, D), BF16), pltpu.VMEM((TOK, D), BF16), jax.ShapeDtypeStruct((D, F), BF16), jax.ShapeDtypeStruct((D, F), BF16), jax.ShapeDtypeStruct((F, D), BF16)),
            in_specs=[hbm] * 14,
            out_specs=(vmem,) * 2 + (hbm,) * 3,
            scratch_shapes=[
                pltpu.VMEM((NSRC, 2, 2, TOP_K, TOK), jnp.int32),
                pltpu.VMEM((NSRC, 2, TOP_K, TOK), F32),
                pltpu.VMEM((2, NSRC, TOK, D), BF16),
                pltpu.VMEM((2, NSRC, EXP, 1, TOK), jnp.int32),
                pltpu.VMEM((2, NSRC, TOK, 3 * EXP * CAP), BF16),
                pltpu.VMEM((GRP, ROWS, D), BF16),
                pltpu.VMEM((2 * TOK, F), BF16),
                pltpu.VMEM((EXP * SIDE, F), BF16),
                pltpu.VMEM((EXP * ROWS, F), BF16),
                pltpu.VMEM((NSRC, EXP, CAP, COL), BF16),
                pltpu.VMEM((4, TOK, COL), F32),
                pltpu.VMEM((steps, TOK, COL), F32),
                pltpu.VMEM((steps, TOK, COL), F32),
                pltpu.VMEM((steps, TOK, COL), F32),
                pltpu.VMEM((SLOTS13, 2, D, F), BF16),
                pltpu.VMEM((SLOTS2, PER, F, COL), BF16),
                sem((2, 4)), sem((2, 2, 3)), sem((2, 2, 3)), sem((2, 3)), sem((2, 3)), sem((2,)), sem((2,)), sem((2, 2)), sem((2, 2)), sem((2, 2)), sem((2, 2)),
                sem((4,)), sem((steps,)), sem((2,)), sem((steps,)), sem((steps,)), sem((steps,)),
                sem((3,)), sem((3,)), sem((3,)), sem((3,)), sem((SLOTS13, 2)), sem((SLOTS2,)), sem((NCOL, 2)),
            ],
            compiler_params=pltpu.CompilerParams(collective_id=0, has_side_effects=True, vmem_limit_bytes=67043328 - 1376256),
        )(tokens_a, tokens_b, experts_a.T, experts_b.T, gates_a.T, gates_b.T, slots_a.T, slots_b.T,
          shared_w1, shared_w3, shared_w2, routed_w1, routed_w3, routed_w2)
        return tuple(pl.pallas_call(
            hand_over,
            name="hand_over",
            out_shape=(tok, tok),
            in_specs=[vmem] * 2,
            out_specs=(hbm,) * 2,
            scratch_shapes=[sem((2,))],
        )(*[pltpu.with_memory_space_constraint(o, pltpu.VMEM) for o in out[:2]]))

    return jax.shard_map(layer_local, mesh=mesh, in_specs=in_specs, out_specs=(tok_spec, tok_spec), check_vma=False)
```

```python
import functools

import jax
import jax.numpy as jnp
from jax import lax
from jax.experimental import pallas as pl
from jax.experimental.pallas import tpu as pltpu
from jax.sharding import PartitionSpec as P

MESH = pl.DeviceIdType.MESH
BF16 = jnp.bfloat16
F32 = jnp.float32

TOK = 256
D = 1280
F = 896
TOP_K = 6
CAP = 48
EXP = 16
NSRC = 4
XP, DG, OWN, CP = range(NSRC)
GRP = 4
COL = 256
NCOL = D // COL
ROWS = NSRC * CAP
SIDE = 2 * CAP
SLOTS13 = 4
SLOTS2 = 5
PER = 4
BLOCKS = EXP // PER


def dot(a, b):
    return jnp.dot(a, b, preferred_element_type=F32)


def kernel(xa, xb, ea, eb, ga, gb, sa, sb, sw1, sw3, sw2, rw1, rw3, rw2,
           oa, ob, pw1, pw3, pw2,
           raw, ids, gates, tokbuf, slots, gmat, rowsg, hs, hfar, hnear, ybuf, work, q0, q2, rr, w13, w2b,
           own_s, meta_s, meta_r, fmeta_s, fmeta_r, tc_s, tc_r, tx_s, tx_r, td_s, td_r, p1_s, p1_r, p3_s, p3_r, rr_s, rr_r,
           yw_s, yw_r, fw_s, fw_r, w13_s, w2_s, sw2_s):
    ep = lax.axis_index("ep")
    tp = lax.axis_index("tp")
    core = lax.rem(ep, 2)
    core_peer = {"ep": ep + 1 - 2 * core}
    x_peer = {"ep": lax.rem(ep + 2, 4)}
    y_peer = {"tp": 1 - tp}
    own = (xa, xb)

    def remote(src, dst, s, r, dev):
        return pltpu.make_async_remote_copy(src_ref=src, dst_ref=dst, send_sem=s, recv_sem=r, device_id=dev, device_id_type=MESH)

    def expert_of(u):
        return lax.rem(jnp.where(u < EXP, u, u + EXP - SLOTS13), EXP)

    def w13_copies(u):
        slot = lax.rem(u, SLOTS13)
        e = expert_of(u)
        return (pltpu.make_async_copy(rw1.at[e], w13.at[slot, 0], w13_s.at[slot, 0]),
                pltpu.make_async_copy(rw3.at[e], w13.at[slot, 1], w13_s.at[slot, 1]))

    def w2_copy(unit):
        slot = lax.rem(unit, SLOTS2)
        n = lax.rem(lax.div(unit, BLOCKS), NCOL)
        first = lax.rem(unit, BLOCKS) * PER
        return pltpu.make_async_copy(rw2.at[pl.ds(first, PER), :, pl.ds(pl.multiple_of(n * COL, COL), COL)], w2b.at[slot], w2_s.at[slot])

    routing = ((ea, sa, ga), (eb, sb, gb))

    def routing_slots(m, src):
        return ids.at[src, m], gates.at[src, m]

    own_cp = [pltpu.make_async_copy(a, b, own_s.at[m, k]) for m in range(2)
              for k, (a, b) in enumerate(zip((*routing[m], own[m]), (raw.at[m, 0], raw.at[m, 1], gates.at[OWN, m], tokbuf.at[m, OWN])))]
    for cp in own_cp:
        cp.start()

    barrier = pltpu.get_barrier_semaphore()
    for dev in (core_peer, x_peer, y_peer):
        pl.semaphore_signal(barrier, inc=1, device_id=dev, device_id_type=MESH)
    pl.semaphore_wait(barrier, 3)
    for cp in own_cp:
        cp.wait()
    for m in range(2):
        ids[OWN, m] = jnp.where(raw[m, 1] >= 0, raw[m, 0] * CAP + raw[m, 1], -1)

    def routing_cp(m, k, src, dst, ss, rs, dev):
        return remote(src[k], routing_slots(m, dst)[k], ss.at[m, k], rs.at[m, k], dev)

    cmeta_cp = [[routing_cp(m, k, routing_slots(m, OWN), CP, meta_s.at[0], meta_r.at[0], core_peer) for k in range(2)] for m in range(2)]
    xmeta_cp = [[routing_cp(m, k, routing_slots(m, OWN), XP, meta_s.at[1], meta_r.at[1], x_peer) for k in range(2)] for m in range(2)]
    dmeta_cp = [[routing_cp(m, k, routing_slots(m, XP), DG, fmeta_s, fmeta_r, core_peer) for k in range(2)] for m in range(2)]
    parts = (pl.ds(0, 3 * TOK // 4), pl.ds(3 * TOK // 4, TOK // 4))
    x_cp = [[remote(tokbuf.at[m, OWN, part], tokbuf.at[m, XP, part], tx_s.at[m, k], tx_r.at[m, k], x_peer) for k, part in enumerate(parts)] for m in range(2)]
    d_cp = [[remote(tokbuf.at[m, XP, part], tokbuf.at[m, DG, part], td_s.at[m, k], td_r.at[m, k], core_peer) for k, part in enumerate(parts)] for m in range(2)]
    c_cp = [remote(tokbuf.at[m, OWN], tokbuf.at[m, CP], tc_s.at[m], tc_r.at[m], core_peer) for m in range(2)]
    for cp in (*xmeta_cp[0], *xmeta_cp[1], *cmeta_cp[0], *cmeta_cp[1], *x_cp[0], *c_cp):
        cp.start()
    local13 = (pltpu.make_async_copy(sw1, w13.at[SLOTS13 - 1, 0], w13_s.at[SLOTS13 - 1, 0]),
               pltpu.make_async_copy(sw3, w13.at[SLOTS13 - 1, 1], w13_s.at[SLOTS13 - 1, 1]))
    for cp in local13:
        cp.start()
    for u in range(SLOTS13 - 1):
        for cp in w13_copies(jnp.int32(u)):
            cp.start()

    half_d, half_f = D // 2, F // 2
    rows_d = pl.ds(pl.multiple_of(core * half_d, 128), half_d)
    rows_f = pl.ds(pl.multiple_of(core * half_f, 64), half_f)
    yw_cp = [remote(w.at[r], p.at[r], yw_s.at[i], yw_r.at[i], y_peer)
             for i, (w, p, r) in enumerate(((sw1, pw1, rows_d), (sw3, pw3, rows_d), (sw2, pw2, rows_f)))]
    fw_cp = [remote(p.at[r], p.at[r], fw_s.at[i], fw_r.at[i], core_peer)
             for i, (p, r) in enumerate(((pw1, rows_d), (pw3, rows_d), (pw2, rows_f)))]
    for cp in yw_cp:
        cp.start()
    for unit in range(SLOTS2):
        w2_copy(jnp.int32(unit)).start()

    def route(i, carry):
        m, src = carry, i
        first = (ep * EXP + lax.broadcasted_iota(jnp.int32, (EXP, TOK), 0)) * CAP
        row_rows, gate_rows = ids[src, m], gates[src, m]
        slot = jnp.full((EXP, TOK), -1, jnp.int32)
        gate = jnp.zeros((EXP, TOK), F32)
        for j in range(TOP_K):
            place = row_rows[j:j + 1, :] - first
            hit = (place >= 0) & (place < CAP)
            slot = jnp.where(hit, place, slot)
            gate = jnp.where(hit, gate_rows[j:j + 1, :], gate)
        pos = lax.broadcasted_iota(jnp.int32, (CAP, TOK), 0)
        for e in range(EXP):
            slots[m, src, e] = slot[e:e + 1, :]
        part = EXP // 2
        for k in range(2):
            g = jnp.concatenate([jnp.where(pos == slot[e:e + 1, :], gate[e:e + 1, :], 0.0)
                                 for e in range(k * part, (k + 1) * part)], axis=0).T
            hi = g.astype(BF16)
            g = g - hi.astype(F32)
            mid = g.astype(BF16)
            low = (g - mid.astype(F32)).astype(BF16)
            for p, v in enumerate((hi, mid, low)):
                gmat[m, src, :, pl.ds(p * EXP * CAP + k * part * CAP, part * CAP)] = v
        return carry

    def route_all(m):
        for cp in (*xmeta_cp[m], *cmeta_cp[m]):
            cp.wait()
        for cp in dmeta_cp[m]:
            cp.start()
        for cp in dmeta_cp[m]:
            cp.wait()
        lax.fori_loop(0, NSRC, route, jnp.int32(m))

    def arrive(m):
        for k in range(2):
            x_cp[m][k].wait()
            d_cp[m][k].start()

    def swiglu_in(x, w1, w3, store):
        full = F // COL
        for k in range(full):
            cols = pl.ds(k * COL, COL)
            a = dot(x, w1[:, cols])
            b = dot(x, w3[:, cols])
            store(cols, (jax.nn.silu(a) * b).astype(BF16))
        cols = pl.ds(full * COL, F - full * COL)
        ab = dot(x, jnp.concatenate([w1[:, cols], w3[:, cols]], axis=1))
        a, b = ab[:, :F - full * COL], ab[:, F - full * COL:]
        store(cols, (jax.nn.silu(a) * b).astype(BF16))

    def gather(g, places):
        pos = lax.broadcasted_iota(jnp.int32, (CAP, TOK), 0)
        for k, (m, src) in enumerate(places):
            place = jnp.concatenate([jnp.where(pos == slots[m, src, g * GRP + i], 1.0, 0.0) for i in range(GRP)], axis=0).astype(BF16)
            for n in range(NCOL):
                cols = pl.ds(n * COL, COL)
                r = dot(place, tokbuf[m, src, :, cols]).astype(BF16)
                for i in range(GRP):
                    rowsg[i, pl.ds(k * CAP, CAP), cols] = r[i * CAP:(i + 1) * CAP]

    def early():
        gather(0, [(m, src) for m in range(2) for src in (OWN, CP)])

        def expert(i, carry):
            for cp in w13_copies(i):
                cp.wait()
            rows = pl.ds(pl.multiple_of(i * ROWS, ROWS), ROWS)

            def store(cols, v):
                hnear[rows, cols] = v

            swiglu_in(rowsg[i], w13.at[i, 0], w13.at[i, 1], store)
            return carry

        lax.fori_loop(0, GRP, expert, 0)

    def phase1(m, after_gather):
        def run(t, g, all_rows):
            gather(g, [(m, src) for src in ((XP, DG, OWN, CP) if all_rows else (XP, DG))])
            after_gather(t)

            def expert(i, carry):
                u = m * EXP + t * GRP + i
                slot = lax.rem(u, SLOTS13)
                rows = pl.ds(pl.multiple_of((g * GRP + i) * SIDE, SIDE), SIDE)
                near = pl.ds(pl.multiple_of((g * GRP + i) * ROWS + m * SIDE, SIDE), SIDE)

                @pl.when((u >= SLOTS13) & ((u < EXP) | (u >= EXP + SLOTS13)))
                def _():
                    for cp in w13_copies(u):
                        cp.wait()

                def store(cols, v):
                    hfar[rows, cols] = v[:SIDE]
                    if all_rows:
                        hnear[near, cols] = v[SIDE:]

                swiglu_in(rowsg[i] if all_rows else rowsg[i, :SIDE], w13.at[slot, 0], w13.at[slot, 1], store)
                nxt = u + SLOTS13

                @pl.when((nxt < EXP) | ((nxt >= EXP + SLOTS13) & (nxt < 2 * EXP)))
                def _():
                    for cp in w13_copies(nxt):
                        cp.start()
                return carry

            lax.fori_loop(0, GRP, expert, 0)

        def group(t, carry):
            g = lax.rem(t + m * (EXP // GRP - 1), EXP // GRP)

            @pl.when(g == 0)
            def _():
                run(t, g, False)

            @pl.when(g > 0)
            def _():
                run(t, g, True)
            return carry

        lax.fori_loop(0, EXP // GRP, group, 0)

    def expand(step, h, sources, blocks=range(BLOCKS), refills=BLOCKS):
        size = sources * CAP
        for b in blocks:
            w2_copy(step * BLOCKS + b).wait()
        for b in blocks:
            slot = lax.rem(step * BLOCKS + b, SLOTS2)
            for i in range(PER):
                e = b * PER + i
                y = dot(h[e * size:(e + 1) * size, :], w2b[slot, i]).astype(BF16)
                for k in range(sources):
                    ybuf[k, e] = y[k * CAP:(k + 1) * CAP]
            if b < refills:
                w2_copy(step * BLOCKS + b + SLOTS2).start()

    def combine(k, m, src):
        y = ybuf[k].reshape(EXP * CAP, COL)
        n = EXP * CAP
        g = gmat.at[m, src]
        return dot(g[:, :n], y) + dot(g[:, n:2 * n], y) + dot(g[:, 2 * n:], y)

    def far_copies(step):
        par = lax.rem(step, 2)
        return (remote(work.at[par], q2.at[step], p3_s.at[par], p3_r.at[step], core_peer),
                remote(q2.at[step], rr.at[step], rr_s.at[step], rr_r.at[step], x_peer))

    def near_copy(m, n):
        return remote(work.at[2 * lax.rem(n, 2) + m], q0.at[m * NCOL + n], p1_s.at[2 * lax.rem(n, 2) + m], p1_r.at[m * NCOL + n], core_peer)

    def finish(step):
        cp, back = far_copies(step)
        cp.wait()
        q2[step] = q2[step] + work[2 + lax.rem(step, 2)]
        back.start()

    def far(m, during):
        def column(n, carry):
            step = m * NCOL + n
            expand(step, hfar, 2, range(BLOCKS // 2))

            if m:
                @pl.when(n == 1)
                def _():
                    finish(step - 1)

            expand(step, hfar, 2, range(BLOCKS // 2, BLOCKS))
            par = lax.rem(step, 2)
            work[par] = combine(DG, m, DG)
            work[2 + par] = combine(XP, m, XP)
            far_copies(step)[0].start()

            during(n)

            @pl.when(n >= 1 + m)
            def _():
                finish(step - 1)
            return carry

        lax.fori_loop(0, NCOL, column, 0)

    def shared_in(half, slot):
        for m in range(2):
            def store(cols, v):
                hs_of(half, m)[:, cols] = v

            swiglu_in(tokbuf[m, OWN], w13.at[slot, 0], w13.at[slot, 1], store)

    def hs_of(half, m):
        rows = pl.ds(m * TOK, TOK)
        return hfar.at[rows, :] if half else hs.at[rows, :]

    for cp in local13:
        cp.wait()
    shared_in(0, SLOTS13 - 1)
    for cp in w13_copies(jnp.int32(SLOTS13 - 1)):
        cp.start()
    route_all(0)
    route_all(1)
    for cp in c_cp:
        cp.wait()
    early()
    arrive(0)
    for cp in x_cp[1]:
        cp.start()
    for cp in d_cp[0]:
        cp.wait()
    phase1(0, lambda t: None)
    arrive(1)
    far(0, lambda n: None)
    for cp in d_cp[1]:
        cp.wait()

    def between(t):
        @pl.when(t == 1)
        def _():
            finish(jnp.int32(NCOL - 1))

        @pl.when(t == 2)
        def _():
            for i in range(2):
                yw_cp[i].wait()
                fw_cp[i].start()

    phase1(1, between)

    peer13 = (pltpu.make_async_copy(pw1, w13.at[1, 0], w13_s.at[1, 0]), pltpu.make_async_copy(pw3, w13.at[1, 1], w13_s.at[1, 1]))

    def sw2_slot(half, n):
        return w13.at[2 + half, lax.div(n, 3), pl.ds(0, F), pl.ds(pl.multiple_of(lax.rem(n, 3) * COL, COL), COL)]

    def sw2_copy(half, n):
        return pltpu.make_async_copy((sw2, pw2)[half].at[:, pl.ds(pl.multiple_of(n * COL, COL), COL)], sw2_slot(half, n), sw2_s.at[n, half])


    def fetch_peer(n):
        for i in range(2):
            @pl.when(n == 2 + i)
            def _():
                fw_cp[i].wait()
                peer13[i].start()

        @pl.when(n == 3)
        def _():
            yw_cp[2].wait()
            fw_cp[2].start()

    far(1, fetch_peer)
    for n in range(NCOL):
        sw2_copy(0, jnp.int32(n)).start()
    fw_cp[2].wait()
    for n in range(NCOL):
        sw2_copy(1, jnp.int32(n)).start()
    for cp in peer13:
        cp.wait()
    shared_in(1, 1)
    finish(jnp.int32(2 * NCOL - 1))

    def near_finish(n):
        for m in range(2):
            step = m * NCOL + n
            near_copy(m, n).wait()
            back = far_copies(step)[1]
            back.wait_recv()
            if m:
                back.wait_send()
            mine = q2[2 * lax.rem(n, 2) + m]
            (oa, ob)[m][:, pl.ds(pl.multiple_of(n * COL, COL), COL)] = (q0[step] + rr[step] + mine).astype(BF16)

    for n in range(NCOL):
        far_copies(jnp.int32(n))[1].wait_send()

    def near_column(n, carry, refills=BLOCKS, final=False):
        for half in range(2):
            sw2_copy(half, n).wait()
        expand(2 * NCOL + n, hnear, NSRC, refills=refills)
        base = 2 * lax.rem(n, 2)
        cols = pl.ds(pl.multiple_of(n * COL, COL), COL)
        for m in range(2):
            work[base + m] = combine(2 * m + 1, m, CP)
        if final:
            for m in range(2):
                near_copy(m, n).start()
        for m in range(2):
            s = dot(jnp.concatenate([hs_of(half, m)[...] for half in range(2)], axis=1),
                    jnp.concatenate([sw2_slot(half, n)[...] for half in range(2)], axis=0))
            q2[base + m] = s + tokbuf[m, OWN, :, cols].astype(F32) + combine(2 * m, m, OWN)
        if not final:
            for m in range(2):
                near_copy(m, n).start()

        @pl.when(n >= 1)
        def _():
            near_finish(n - 1)
        return carry

    last = NCOL * BLOCKS * 3 - SLOTS2
    full = (last - 2 * NCOL * BLOCKS) // BLOCKS
    lax.fori_loop(0, full, near_column, 0)
    for n in range(full, NCOL):
        near_column(jnp.int32(n), 0, max(0, last - (2 * NCOL + n) * BLOCKS), n == NCOL - 1)
    near_finish(jnp.int32(NCOL - 1))


def hand_over(a, b, oa, ob, out_s):
    copies = [pltpu.make_async_copy(src, dst, out_s.at[m]) for m, (src, dst) in enumerate(((a, oa), (b, ob)))]
    for cp in copies:
        cp.start()
    for cp in copies:
        cp.wait()


def solution(mesh):
    tok_spec = P(('data', 'ep', 'tp'), None)
    in_specs = (tok_spec,) * 8 + (P(None, 'tp'), P(None, 'tp'), P('tp', None), P('ep', None, None), P('ep', None, None), P('ep', None, None))

    def layer_local(tokens_a, tokens_b, experts_a, experts_b, gates_a, gates_b, slots_a, slots_b,
                    shared_w1, shared_w3, shared_w2, routed_w1, routed_w3, routed_w2):
        hbm = pl.BlockSpec(memory_space=pltpu.HBM)
        vmem = pl.BlockSpec(memory_space=pltpu.VMEM)
        sem = pltpu.SemaphoreType.DMA
        steps = 2 * NCOL
        tok = jax.ShapeDtypeStruct((TOK, D), BF16)
        out = pl.pallas_call(
            kernel,
            name="moe_layer",
            out_shape=(pltpu.VMEM((TOK, D), BF16), pltpu.VMEM((TOK, D), BF16), jax.ShapeDtypeStruct((D, F), BF16), jax.ShapeDtypeStruct((D, F), BF16), jax.ShapeDtypeStruct((F, D), BF16)),
            in_specs=[hbm] * 14,
            out_specs=(vmem,) * 2 + (hbm,) * 3,
            scratch_shapes=[
                pltpu.VMEM((2, 2, TOP_K, TOK), jnp.int32),
                pltpu.VMEM((NSRC, 2, TOP_K, TOK), jnp.int32),
                pltpu.VMEM((NSRC, 2, TOP_K, TOK), F32),
                pltpu.VMEM((2, NSRC, TOK, D), BF16),
                pltpu.VMEM((2, NSRC, EXP, 1, TOK), jnp.int32),
                pltpu.VMEM((2, NSRC, TOK, 3 * EXP * CAP), BF16),
                pltpu.VMEM((GRP, ROWS, D), BF16),
                pltpu.VMEM((2 * TOK, F), BF16),
                pltpu.VMEM((EXP * SIDE, F), BF16),
                pltpu.VMEM((EXP * ROWS, F), BF16),
                pltpu.VMEM((NSRC, EXP, CAP, COL), BF16),
                pltpu.VMEM((4, TOK, COL), F32),
                pltpu.VMEM((steps, TOK, COL), F32),
                pltpu.VMEM((steps, TOK, COL), F32),
                pltpu.VMEM((steps, TOK, COL), F32),
                pltpu.VMEM((SLOTS13, 2, D, F), BF16),
                pltpu.VMEM((SLOTS2, PER, F, COL), BF16),
                sem((2, 4)), sem((2, 2, 2)), sem((2, 2, 2)), sem((2, 2)), sem((2, 2)), sem((2,)), sem((2,)), sem((2, 2)), sem((2, 2)), sem((2, 2)), sem((2, 2)),
                sem((4,)), sem((steps,)), sem((2,)), sem((steps,)), sem((steps,)), sem((steps,)),
                sem((3,)), sem((3,)), sem((3,)), sem((3,)), sem((SLOTS13, 2)), sem((SLOTS2,)), sem((NCOL, 2)),
            ],
            compiler_params=pltpu.CompilerParams(collective_id=0, has_side_effects=True, vmem_limit_bytes=67043328 - 1376256),
        )(tokens_a, tokens_b, experts_a.T, experts_b.T, gates_a.T, gates_b.T, slots_a.T, slots_b.T,
          shared_w1, shared_w3, shared_w2, routed_w1, routed_w3, routed_w2)
        return tuple(pl.pallas_call(
            hand_over,
            name="hand_over",
            out_shape=(tok, tok),
            in_specs=[vmem] * 2,
            out_specs=(hbm,) * 2,
            scratch_shapes=[sem((2,))],
        )(*[pltpu.with_memory_space_constraint(o, pltpu.VMEM) for o in out[:2]]))

    return jax.shard_map(layer_local, mesh=mesh, in_specs=in_specs, out_specs=(tok_spec, tok_spec), check_vma=False)
```

```python
import functools

import jax
import jax.numpy as jnp
from jax import lax
from jax.experimental import pallas as pl
from jax.experimental.pallas import tpu as pltpu
from jax.sharding import PartitionSpec as P

MESH = pl.DeviceIdType.MESH
BF16 = jnp.bfloat16
F32 = jnp.float32

TOK = 256
D = 1280
F = 896
TOP_K = 6
CAP = 48
EXP = 16
NSRC = 4
XP, DG, OWN, CP = range(NSRC)
GRP = 4
COL = 256
NCOL = D // COL
ROWS = NSRC * CAP
SIDE = 2 * CAP
SLOTS13 = 4
SLOTS2 = 5
PER = 4
BLOCKS = EXP // PER


def dot(a, b):
    return jnp.dot(a, b, preferred_element_type=F32)


def kernel(xa, xb, ea, eb, ga, gb, sa, sb, sw1, sw3, sw2, rw1, rw3, rw2,
           oa, ob, pw1, pw3, pw2,
           raw, ids, gates, tokbuf, slots, gmat, rowsg, hs, hfar, hnear, ybuf, work, q0, q2, rr, w13, w2b,
           own_s, meta_s, meta_r, fmeta_s, fmeta_r, tc_s, tc_r, tx_s, tx_r, td_s, td_r, p1_s, p1_r, p3_s, p3_r, rr_s, rr_r,
           yw_s, yw_r, fw_s, fw_r, w13_s, w2_s, sw2_s):
    ep = lax.axis_index("ep")
    tp = lax.axis_index("tp")
    core = lax.rem(ep, 2)
    core_peer = {"ep": ep + 1 - 2 * core}
    x_peer = {"ep": lax.rem(ep + 2, 4)}
    y_peer = {"tp": 1 - tp}
    own = (xa, xb)

    def remote(src, dst, s, r, dev):
        return pltpu.make_async_remote_copy(src_ref=src, dst_ref=dst, send_sem=s, recv_sem=r, device_id=dev, device_id_type=MESH)

    def expert_of(u):
        return lax.rem(jnp.where(u < EXP, u, u + EXP - SLOTS13), EXP)

    def w13_copies(u):
        slot = lax.rem(u, SLOTS13)
        e = expert_of(u)
        return (pltpu.make_async_copy(rw1.at[e], w13.at[slot, 0], w13_s.at[slot, 0]),
                pltpu.make_async_copy(rw3.at[e], w13.at[slot, 1], w13_s.at[slot, 1]))

    def w2_copy(unit):
        slot = lax.rem(unit, SLOTS2)
        n = lax.rem(lax.div(unit, BLOCKS), NCOL)
        first = lax.rem(unit, BLOCKS) * PER
        return pltpu.make_async_copy(rw2.at[pl.ds(first, PER), :, pl.ds(pl.multiple_of(n * COL, COL), COL)], w2b.at[slot], w2_s.at[slot])

    routing = ((ea, sa, ga), (eb, sb, gb))

    def routing_slots(m, src):
        return ids.at[src, m], gates.at[src, m]

    own_cp = [pltpu.make_async_copy(a, b, own_s.at[m, k]) for m in range(2)
              for k, (a, b) in enumerate(zip((*routing[m], own[m]), (raw.at[m, 0], raw.at[m, 1], gates.at[OWN, m], tokbuf.at[m, OWN])))]
    for cp in own_cp:
        cp.start()

    barrier = pltpu.get_barrier_semaphore()
    for dev in (core_peer, x_peer, y_peer):
        pl.semaphore_signal(barrier, inc=1, device_id=dev, device_id_type=MESH)
    pl.semaphore_wait(barrier, 3)
    for cp in own_cp:
        cp.wait()
    for m in range(2):
        ids[OWN, m] = jnp.where(raw[m, 1] >= 0, raw[m, 0] * CAP + raw[m, 1], -1)

    def routing_cp(m, k, src, dst, ss, rs, dev):
        return remote(src[k], routing_slots(m, dst)[k], ss.at[m, k], rs.at[m, k], dev)

    cmeta_cp = [[routing_cp(m, k, routing_slots(m, OWN), CP, meta_s.at[0], meta_r.at[0], core_peer) for k in range(2)] for m in range(2)]
    xmeta_cp = [[routing_cp(m, k, routing_slots(m, OWN), XP, meta_s.at[1], meta_r.at[1], x_peer) for k in range(2)] for m in range(2)]
    dmeta_cp = [[routing_cp(m, k, routing_slots(m, XP), DG, fmeta_s, fmeta_r, core_peer) for k in range(2)] for m in range(2)]
    parts = (pl.ds(0, 7 * TOK // 8), pl.ds(7 * TOK // 8, TOK // 8))
    x_cp = [[remote(tokbuf.at[m, OWN, part], tokbuf.at[m, XP, part], tx_s.at[m, k], tx_r.at[m, k], x_peer) for k, part in enumerate(parts)] for m in range(2)]
    d_cp = [[remote(tokbuf.at[m, XP, part], tokbuf.at[m, DG, part], td_s.at[m, k], td_r.at[m, k], core_peer) for k, part in enumerate(parts)] for m in range(2)]
    c_cp = [remote(tokbuf.at[m, OWN], tokbuf.at[m, CP], tc_s.at[m], tc_r.at[m], core_peer) for m in range(2)]
    for cp in (*xmeta_cp[0], *xmeta_cp[1], *cmeta_cp[0], *cmeta_cp[1], *x_cp[0], *c_cp):
        cp.start()
    local13 = (pltpu.make_async_copy(sw1, w13.at[SLOTS13 - 1, 0], w13_s.at[SLOTS13 - 1, 0]),
               pltpu.make_async_copy(sw3, w13.at[SLOTS13 - 1, 1], w13_s.at[SLOTS13 - 1, 1]))
    for cp in local13:
        cp.start()
    for u in range(SLOTS13 - 1):
        for cp in w13_copies(jnp.int32(u)):
            cp.start()

    half_d, half_f = D // 2, F // 2
    rows_d = pl.ds(pl.multiple_of(core * half_d, 128), half_d)
    rows_f = pl.ds(pl.multiple_of(core * half_f, 64), half_f)
    yw_cp = [remote(w.at[r], p.at[r], yw_s.at[i], yw_r.at[i], y_peer)
             for i, (w, p, r) in enumerate(((sw1, pw1, rows_d), (sw3, pw3, rows_d), (sw2, pw2, rows_f)))]
    fw_cp = [remote(p.at[r], p.at[r], fw_s.at[i], fw_r.at[i], core_peer)
             for i, (p, r) in enumerate(((pw1, rows_d), (pw3, rows_d), (pw2, rows_f)))]
    for cp in yw_cp:
        cp.start()
    for unit in range(SLOTS2):
        w2_copy(jnp.int32(unit)).start()

    def route(i, carry):
        m, src = carry, i
        first = (ep * EXP + lax.broadcasted_iota(jnp.int32, (EXP, TOK), 0)) * CAP
        row_rows, gate_rows = ids[src, m], gates[src, m]
        slot = jnp.full((EXP, TOK), -1, jnp.int32)
        gate = jnp.zeros((EXP, TOK), F32)
        for j in range(TOP_K):
            place = row_rows[j:j + 1, :] - first
            hit = (place >= 0) & (place < CAP)
            slot = jnp.where(hit, place, slot)
            gate = jnp.where(hit, gate_rows[j:j + 1, :], gate)
        pos = lax.broadcasted_iota(jnp.int32, (CAP, TOK), 0)
        for e in range(EXP):
            slots[m, src, e] = slot[e:e + 1, :]
        part = EXP // 2
        for k in range(2):
            g = jnp.concatenate([jnp.where(pos == slot[e:e + 1, :], gate[e:e + 1, :], 0.0)
                                 for e in range(k * part, (k + 1) * part)], axis=0).T
            hi = g.astype(BF16)
            g = g - hi.astype(F32)
            mid = g.astype(BF16)
            low = (g - mid.astype(F32)).astype(BF16)
            for p, v in enumerate((hi, mid, low)):
                gmat[m, src, :, pl.ds(p * EXP * CAP + k * part * CAP, part * CAP)] = v
        return carry

    def route_all(m):
        for cp in (*xmeta_cp[m], *cmeta_cp[m]):
            cp.wait()
        for cp in dmeta_cp[m]:
            cp.start()
        for cp in dmeta_cp[m]:
            cp.wait()
        lax.fori_loop(0, NSRC, route, jnp.int32(m))

    def arrive(m):
        for k in range(2):
            x_cp[m][k].wait()
            d_cp[m][k].start()

    def swiglu_in(x, w1, w3, store):
        full = F // COL
        for k in range(full):
            cols = pl.ds(k * COL, COL)
            a = dot(x, w1[:, cols])
            b = dot(x, w3[:, cols])
            store(cols, (jax.nn.silu(a) * b).astype(BF16))
        cols = pl.ds(full * COL, F - full * COL)
        ab = dot(x, jnp.concatenate([w1[:, cols], w3[:, cols]], axis=1))
        a, b = ab[:, :F - full * COL], ab[:, F - full * COL:]
        store(cols, (jax.nn.silu(a) * b).astype(BF16))

    def gather(g, places):
        pos = lax.broadcasted_iota(jnp.int32, (CAP, TOK), 0)
        for k, (m, src) in enumerate(places):
            place = jnp.concatenate([jnp.where(pos == slots[m, src, g * GRP + i], 1.0, 0.0) for i in range(GRP)], axis=0).astype(BF16)
            for n in range(NCOL):
                cols = pl.ds(n * COL, COL)
                r = dot(place, tokbuf[m, src, :, cols]).astype(BF16)
                for i in range(GRP):
                    rowsg[i, pl.ds(k * CAP, CAP), cols] = r[i * CAP:(i + 1) * CAP]

    def early():
        gather(0, [(m, src) for m in range(2) for src in (OWN, CP)])

        def expert(i, carry):
            for cp in w13_copies(i):
                cp.wait()
            rows = pl.ds(pl.multiple_of(i * ROWS, ROWS), ROWS)

            def store(cols, v):
                hnear[rows, cols] = v

            swiglu_in(rowsg[i], w13.at[i, 0], w13.at[i, 1], store)
            return carry

        lax.fori_loop(0, GRP, expert, 0)

    def phase1(m, after_gather):
        def run(t, g, all_rows):
            gather(g, [(m, src) for src in ((XP, DG, OWN, CP) if all_rows else (XP, DG))])
            after_gather(t)

            def expert(i, carry):
                u = m * EXP + t * GRP + i
                slot = lax.rem(u, SLOTS13)
                rows = pl.ds(pl.multiple_of((g * GRP + i) * SIDE, SIDE), SIDE)
                near = pl.ds(pl.multiple_of((g * GRP + i) * ROWS + m * SIDE, SIDE), SIDE)

                @pl.when((u >= SLOTS13) & ((u < EXP) | (u >= EXP + SLOTS13)))
                def _():
                    for cp in w13_copies(u):
                        cp.wait()

                def store(cols, v):
                    hfar[rows, cols] = v[:SIDE]
                    if all_rows:
                        hnear[near, cols] = v[SIDE:]

                swiglu_in(rowsg[i] if all_rows else rowsg[i, :SIDE], w13.at[slot, 0], w13.at[slot, 1], store)
                nxt = u + SLOTS13

                @pl.when((nxt < EXP) | ((nxt >= EXP + SLOTS13) & (nxt < 2 * EXP)))
                def _():
                    for cp in w13_copies(nxt):
                        cp.start()
                return carry

            lax.fori_loop(0, GRP, expert, 0)

        def group(t, carry):
            g = lax.rem(t + m * (EXP // GRP - 1), EXP // GRP)

            @pl.when(g == 0)
            def _():
                run(t, g, False)

            @pl.when(g > 0)
            def _():
                run(t, g, True)
            return carry

        lax.fori_loop(0, EXP // GRP, group, 0)

    def expand(step, h, sources, blocks=range(BLOCKS), refills=BLOCKS):
        size = sources * CAP
        for b in blocks:
            w2_copy(step * BLOCKS + b).wait()
        for b in blocks:
            slot = lax.rem(step * BLOCKS + b, SLOTS2)
            for i in range(PER):
                e = b * PER + i
                y = dot(h[e * size:(e + 1) * size, :], w2b[slot, i]).astype(BF16)
                for k in range(sources):
                    ybuf[k, e] = y[k * CAP:(k + 1) * CAP]
            if b < refills:
                w2_copy(step * BLOCKS + b + SLOTS2).start()

    def combine(k, m, src):
        y = ybuf[k].reshape(EXP * CAP, COL)
        n = EXP * CAP
        g = gmat.at[m, src]
        return dot(g[:, :n], y) + dot(g[:, n:2 * n], y) + dot(g[:, 2 * n:], y)

    def far_copies(step):
        par = lax.rem(step, 2)
        return (remote(work.at[par], q2.at[step], p3_s.at[par], p3_r.at[step], core_peer),
                remote(q2.at[step], rr.at[step], rr_s.at[step], rr_r.at[step], x_peer))

    def near_copy(m, n):
        return remote(work.at[2 * lax.rem(n, 2) + m], q0.at[m * NCOL + n], p1_s.at[2 * lax.rem(n, 2) + m], p1_r.at[m * NCOL + n], core_peer)

    def finish(step):
        cp, back = far_copies(step)
        cp.wait()
        q2[step] = q2[step] + work[2 + lax.rem(step, 2)]
        back.start()

    def far(m, during):
        def column(n, carry):
            step = m * NCOL + n
            expand(step, hfar, 2, range(BLOCKS // 2))

            if m:
                @pl.when(n == 1)
                def _():
                    finish(step - 1)

            expand(step, hfar, 2, range(BLOCKS // 2, BLOCKS))
            par = lax.rem(step, 2)
            work[par] = combine(DG, m, DG)
            work[2 + par] = combine(XP, m, XP)
            far_copies(step)[0].start()

            during(n)

            @pl.when(n >= 1 + m)
            def _():
                finish(step - 1)
            return carry

        lax.fori_loop(0, NCOL, column, 0)

    def shared_in(half, slot):
        for m in range(2):
            def store(cols, v):
                hs_of(half, m)[:, cols] = v

            swiglu_in(tokbuf[m, OWN], w13.at[slot, 0], w13.at[slot, 1], store)

    def hs_of(half, m):
        rows = pl.ds(m * TOK, TOK)
        return hfar.at[rows, :] if half else hs.at[rows, :]

    for cp in local13:
        cp.wait()
    shared_in(0, SLOTS13 - 1)
    for cp in w13_copies(jnp.int32(SLOTS13 - 1)):
        cp.start()
    route_all(0)
    route_all(1)
    for cp in c_cp:
        cp.wait()
    early()
    arrive(0)
    for cp in x_cp[1]:
        cp.start()
    for cp in d_cp[0]:
        cp.wait()
    phase1(0, lambda t: None)
    arrive(1)
    far(0, lambda n: None)
    for cp in d_cp[1]:
        cp.wait()

    def between(t):
        @pl.when(t == 1)
        def _():
            finish(jnp.int32(NCOL - 1))

        @pl.when(t == 2)
        def _():
            for i in range(2):
                yw_cp[i].wait()
                fw_cp[i].start()

    phase1(1, between)

    peer13 = (pltpu.make_async_copy(pw1, w13.at[1, 0], w13_s.at[1, 0]), pltpu.make_async_copy(pw3, w13.at[1, 1], w13_s.at[1, 1]))

    def sw2_slot(half, n):
        return w13.at[2 + half, lax.div(n, 3), pl.ds(0, F), pl.ds(pl.multiple_of(lax.rem(n, 3) * COL, COL), COL)]

    def sw2_copies(half):
        return [pltpu.make_async_copy((sw2, pw2)[half].at[:, pl.ds(3 * k * COL, width)],
                                      w13.at[2 + half, k, pl.ds(0, F), pl.ds(0, width)], sw2_s.at[half, k])
                for k, width in enumerate((3 * COL, (NCOL - 3) * COL))]

    def fetch_peer(n):
        for i in range(2):
            @pl.when(n == 2 + i)
            def _():
                fw_cp[i].wait()
                peer13[i].start()

        @pl.when(n == 3)
        def _():
            yw_cp[2].wait()
            fw_cp[2].start()

    far(1, fetch_peer)
    for cp in sw2_copies(0):
        cp.start()
    fw_cp[2].wait()
    for cp in sw2_copies(1):
        cp.start()
    for cp in peer13:
        cp.wait()
    shared_in(1, 1)
    finish(jnp.int32(2 * NCOL - 1))

    def near_finish(n):
        for m in range(2):
            step = m * NCOL + n
            near_copy(m, n).wait()
            back = far_copies(step)[1]
            back.wait_recv()
            if m:
                back.wait_send()
            mine = q2[2 * lax.rem(n, 2) + m]
            (oa, ob)[m][:, pl.ds(pl.multiple_of(n * COL, COL), COL)] = (q0[step] + rr[step] + mine).astype(BF16)

    for n in range(NCOL):
        far_copies(jnp.int32(n))[1].wait_send()

    for cp in (*sw2_copies(0), *sw2_copies(1)):
        cp.wait()

    def near_column(n, carry, refills=BLOCKS, final=False):
        expand(2 * NCOL + n, hnear, NSRC, refills=refills)
        base = 2 * lax.rem(n, 2)
        cols = pl.ds(pl.multiple_of(n * COL, COL), COL)
        for m in range(2):
            work[base + m] = combine(2 * m + 1, m, CP)
        if final:
            for m in range(2):
                near_copy(m, n).start()
        for m in range(2):
            s = dot(jnp.concatenate([hs_of(half, m)[...] for half in range(2)], axis=1),
                    jnp.concatenate([sw2_slot(half, n)[...] for half in range(2)], axis=0))
            q2[base + m] = s + tokbuf[m, OWN, :, cols].astype(F32) + combine(2 * m, m, OWN)
        if not final:
            for m in range(2):
                near_copy(m, n).start()

        @pl.when(n >= 1)
        def _():
            near_finish(n - 1)
        return carry

    last = NCOL * BLOCKS * 3 - SLOTS2
    full = (last - 2 * NCOL * BLOCKS) // BLOCKS
    lax.fori_loop(0, full, near_column, 0)
    for n in range(full, NCOL):
        near_column(jnp.int32(n), 0, max(0, last - (2 * NCOL + n) * BLOCKS), n == NCOL - 1)
    near_finish(jnp.int32(NCOL - 1))


def hand_over(a, b, oa, ob, out_s):
    copies = [pltpu.make_async_copy(src, dst, out_s.at[m]) for m, (src, dst) in enumerate(((a, oa), (b, ob)))]
    for cp in copies:
        cp.start()
    for cp in copies:
        cp.wait()


def solution(mesh):
    tok_spec = P(('data', 'ep', 'tp'), None)
    in_specs = (tok_spec,) * 8 + (P(None, 'tp'), P(None, 'tp'), P('tp', None), P('ep', None, None), P('ep', None, None), P('ep', None, None))

    def layer_local(tokens_a, tokens_b, experts_a, experts_b, gates_a, gates_b, slots_a, slots_b,
                    shared_w1, shared_w3, shared_w2, routed_w1, routed_w3, routed_w2):
        hbm = pl.BlockSpec(memory_space=pltpu.HBM)
        vmem = pl.BlockSpec(memory_space=pltpu.VMEM)
        sem = pltpu.SemaphoreType.DMA
        steps = 2 * NCOL
        tok = jax.ShapeDtypeStruct((TOK, D), BF16)
        out = pl.pallas_call(
            kernel,
            name="moe_layer",
            out_shape=(pltpu.VMEM((TOK, D), BF16), pltpu.VMEM((TOK, D), BF16), jax.ShapeDtypeStruct((D, F), BF16), jax.ShapeDtypeStruct((D, F), BF16), jax.ShapeDtypeStruct((F, D), BF16)),
            in_specs=[hbm] * 14,
            out_specs=(vmem,) * 2 + (hbm,) * 3,
            scratch_shapes=[
                pltpu.VMEM((2, 2, TOP_K, TOK), jnp.int32),
                pltpu.VMEM((NSRC, 2, TOP_K, TOK), jnp.int32),
                pltpu.VMEM((NSRC, 2, TOP_K, TOK), F32),
                pltpu.VMEM((2, NSRC, TOK, D), BF16),
                pltpu.VMEM((2, NSRC, EXP, 1, TOK), jnp.int32),
                pltpu.VMEM((2, NSRC, TOK, 3 * EXP * CAP), BF16),
                pltpu.VMEM((GRP, ROWS, D), BF16),
                pltpu.VMEM((2 * TOK, F), BF16),
                pltpu.VMEM((EXP * SIDE, F), BF16),
                pltpu.VMEM((EXP * ROWS, F), BF16),
                pltpu.VMEM((NSRC, EXP, CAP, COL), BF16),
                pltpu.VMEM((4, TOK, COL), F32),
                pltpu.VMEM((steps, TOK, COL), F32),
                pltpu.VMEM((steps, TOK, COL), F32),
                pltpu.VMEM((steps, TOK, COL), F32),
                pltpu.VMEM((SLOTS13, 2, D, F), BF16),
                pltpu.VMEM((SLOTS2, PER, F, COL), BF16),
                sem((2, 4)), sem((2, 2, 2)), sem((2, 2, 2)), sem((2, 2)), sem((2, 2)), sem((2,)), sem((2,)), sem((2, 2)), sem((2, 2)), sem((2, 2)), sem((2, 2)),
                sem((4,)), sem((steps,)), sem((2,)), sem((steps,)), sem((steps,)), sem((steps,)),
                sem((3,)), sem((3,)), sem((3,)), sem((3,)), sem((SLOTS13, 2)), sem((SLOTS2,)), sem((2, 2)),
            ],
            compiler_params=pltpu.CompilerParams(collective_id=0, has_side_effects=True, vmem_limit_bytes=67043328 - 1376256),
        )(tokens_a, tokens_b, experts_a.T, experts_b.T, gates_a.T, gates_b.T, slots_a.T, slots_b.T,
          shared_w1, shared_w3, shared_w2, routed_w1, routed_w3, routed_w2)
        return tuple(pl.pallas_call(
            hand_over,
            name="hand_over",
            out_shape=(tok, tok),
            in_specs=[vmem] * 2,
            out_specs=(hbm,) * 2,
            scratch_shapes=[sem((2,))],
        )(*[pltpu.with_memory_space_constraint(o, pltpu.VMEM) for o in out[:2]]))

    return jax.shard_map(layer_local, mesh=mesh, in_specs=in_specs, out_specs=(tok_spec, tok_spec), check_vma=False)
```
